128 devices in a mesh: gx: 4 (over x), gy: 4 (over y), gz: 8 (over z, core).
Axes of the slice: x: 4, y: 4, z: 4, core: 2. Of those that a mesh axis runs over, the one named last changes fastest.
Arguments:
- seg_rows: bfloat16 [16384, 128, 128], P(('gx', 'gy', 'gz')), may hold values from -6 to 6
- owner_map: int32 [16384, 1], replicated, may hold values from 0 to 127; in each aligned block of 128 rows (0 to 127, 128 to 255, ...) at most 2 rows name the same one
- ghost_pick: int32 [128, 1], P(('gx', 'gy', 'gz')), may hold values from 0 to 127
- slab_cost: int32 [4, 4, 8, 3, 1024], P('gx', 'gy', 'gz'), may hold values from 1 to 24
Outputs:
- forces: bfloat16 [128, 128, 2, 128, 128], P(('gx', 'gy', 'gz'))
- cut_points: float32 [7], replicated
The draws below stay inside these ranges and needn't reach their ends.
Inputs may be any that keep to these rules, and one draw needn't show every extreme that they name: `owner_map`: among the 128 blocks of one device (aligned runs of 128 rows) no owner is named more than 2 times; some device names some owner exactly 2 times.
All inputs are finite; a program needn't handle non-finite values.
Results may differ from the reference program's by a relative error of at most 0.0034.
Values may be sent and summed in bfloat16 or wider, within the bound.
No kernel may reach another device: no remote copies, remote signals or barrier semaphores. Data moves between devices by JAX's collectives and lax.ppermute only.
A program may use at most 128 MiB of HBM per device.

```python
import math
import jax
import jax.numpy as jnp
import numpy as np
from jax import lax

W = 128
BLK = 128
BLK_DEV = 128
GH = 1
NSLAB = 1024
BLOCKS = 16384
CAP = 2
N_GX = 4
N_GY = 4
N_GZ = 8
DEVICES = 128


def draw_slab_cost(key, part):
    full_shape = (N_GX, N_GY, N_GZ, 3, NSLAB)
    coord_x = lax.broadcasted_iota(jnp.int32, full_shape, 0)
    coord_y = lax.broadcasted_iota(jnp.int32, full_shape, 1)
    coord_z = lax.broadcasted_iota(jnp.int32, full_shape, 2)
    direction = lax.broadcasted_iota(jnp.int32, full_shape, 3)
    slab_index = lax.broadcasted_iota(jnp.int32, full_shape, 4)
    flat_dev = (coord_x * N_GY + coord_y) * N_GZ + coord_z
    own_coord = jnp.where(direction == 0, coord_x, jnp.where(direction == 1, coord_y, coord_z))
    extent = jnp.where(direction == 0, N_GX, jnp.where(direction == 1, N_GY, N_GZ))
    region = slab_index * extent // NSLAB
    hot_key = jax.random.fold_in(key, 11)
    cost_key = jax.random.fold_in(key, 23)
    hotness = jax.random.randint(hot_key, (N_GX, N_GY, N_GZ, 3, 1), 1, 9, dtype=jnp.int32)
    ceiling = jnp.where(region == own_coord, 1 + hotness * (DEVICES + 2 * flat_dev) // DEVICES, 1)
    return jax.random.randint(cost_key, full_shape, 1, ceiling + 1, dtype=jnp.int32)


def place_ends(values, own_key, smallest, high):
    index_at = [jax.random.randint(jax.random.fold_in(own_key, axis), (), 0, length) for axis, length in enumerate(values.shape)]
    widest = values.shape.index(max(values.shape))
    beside = index_at[:widest] + [(index_at[widest] + 1) % values.shape[widest]] + index_at[widest + 1:]
    return values.at[tuple(index_at)].set(smallest).at[tuple(beside)].set(high)


def levels(own_key, shape, pieces, least, largest):
    loudness, own = 1.0, jax.random.fold_in(own_key, 6)
    for dim, parts in pieces:
        draws = jnp.exp(jax.random.uniform(jax.random.fold_in(own, dim), (parts,), jnp.float32, least / len(pieces), largest / len(pieces)))
        loudness = loudness * jnp.repeat(draws, shape[dim] // parts).reshape([-1 if axis == dim else 1 for axis in range(len(shape))])
    return loudness


def deal_out(key, own, number, rows, count, top, most, skew):
    ranking = jax.random.permutation(key, count)
    crowded, common = portions_of(count, rows * top, most, skew, True), portions_of(count, rows * top, most, skew, False)
    places = jnp.arange(count)

    def named(sizes, offset_by):
        used = int((sizes > 0).sum())
        fixed = max(1, used // 4)
        passed = fixed + (places - fixed + offset_by * (used - fixed)) % max(1, count - fixed)
        return jnp.zeros((count,), jnp.int32).at[ranking[jnp.where(places < fixed, places, passed)]].set(jnp.asarray(sizes, jnp.int32))

    sizes = jnp.where(number % 4 == 0, named(crowded, number // 4), named(common, number - number // 4 - 1))
    mixed = jax.random.permutation(jax.random.fold_in(own, 3), count)
    source_of, receiver = mixed[0:count // 2 * 2:2], mixed[1:count // 2 * 2:2]
    slack = jnp.minimum(sizes[source_of] - 1, most - sizes[receiver]) // 2
    slack = jnp.where((source_of == ranking[0]) | (receiver == ranking[0]) | (sizes[receiver] == 0), 0, jnp.maximum(slack, 0))
    passed = jax.random.randint(jax.random.fold_in(own, 4), (count // 2,), 0, 1 << 20) % (slack + 1)
    sizes = sizes.at[source_of].add(-passed).at[receiver].add(passed)
    labels = jnp.searchsorted(jnp.cumsum(sizes), jnp.arange(rows * top), side="right").astype(jnp.int32)
    listing = labels.reshape(top, rows).T
    listing = listing[jax.random.permutation(jax.random.fold_in(own, 1), rows)]
    offset_by = jax.random.randint(jax.random.fold_in(own, 2), (rows, 1), 0, top)
    return jnp.take_along_axis(listing, (jnp.arange(top)[None, :] + offset_by) % top, axis=1)


def portions_of(count, total, limit, lean, full):
    loads = [(1 << 20) // math.isqrt(rank ** lean) + 1 for rank in range(1, count + 1)]
    largest = limit if full else min(limit, max(-(-total // count), total * loads[0] // sum(loads)))
    least = 1 if total - largest >= count - 1 else 0
    holding, spare = [largest] + [least] * (count - 1), total - largest - least * (count - 1)
    while spare > 0:
        movable = [i for i in range(1, count) if holding[i] < largest] or [i for i in range(1, count) if holding[i] < limit]
        whole, left = sum([loads[i] for i in movable]), spare
        for i in movable:
            more = min(limit - holding[i], max(1, left * loads[i] // whole), spare)
            holding[i] = holding[i] + more
            spare = spare - more
    return np.array(holding)


def noise(key, shape, scale, limit, split=(), kind=jnp.bfloat16):
    factor_of = levels(key, shape, split, -0.22, 0.18) if split else 1.0
    values = jax.random.normal(key, shape, jnp.float32) * scale * factor_of
    return jnp.minimum(jnp.maximum(values, -limit), limit).astype(kind)


def setup_inputs(seed: int = 0) -> dict:
    keys = jax.random.split(jax.random.key(seed), 5)
    seg_rows = noise(keys[0], (BLOCKS, BLK, W), 1.0, 6.0, ((0, 128),))
    owner_map_keys = jax.random.split(jax.random.fold_in(keys[1], 1), BLOCKS // BLK_DEV)
    owner_map_turns = jax.random.permutation(jax.random.fold_in(keys[1], 3), BLOCKS // BLK_DEV)
    owner_map = jax.vmap(lambda own, number: deal_out(jax.random.fold_in(keys[1], 2), own, number, BLK_DEV, DEVICES, 1, CAP, 2))(owner_map_keys, owner_map_turns).reshape((BLOCKS, 1))
    ghost_pick = place_ends(jax.random.randint(keys[2], (DEVICES, GH), 0, BLK_DEV), jax.random.fold_in(keys[2], 1), 0, BLK_DEV - 1).astype(jnp.int32)
    slab_cost = draw_slab_cost(jax.random.fold_in(keys[4], 71), 0)
    return dict(seg_rows=seg_rows, owner_map=owner_map, ghost_pick=ghost_pick, slab_cost=slab_cost)


sharpness = 8.0
force_gain = 2.0
radius_eps = 1e-3


def bisect_cuts(histogram):
    running = jnp.cumsum(histogram, axis=1, dtype=jnp.int32)
    total_cost = running[:, -1]
    below = (2 * running < total_cost[:, None]).astype(jnp.int32)
    position = jnp.sum(below, axis=1, dtype=jnp.int32)
    before = jnp.sum(histogram * below, axis=1, dtype=jnp.int32)
    bins_index = lax.broadcasted_iota(jnp.int32, histogram.shape, 1)
    at_cut = jnp.sum(jnp.where(bins_index == position[:, None], histogram, 0), axis=1, dtype=jnp.int32)
    remain = (total_cost - 2 * before).astype(jnp.float32)
    return (position.astype(jnp.float32) + remain / (2 * at_cut).astype(jnp.float32)) / histogram.shape[1]


def kernel_weights(left_sq, right_sq, inner):
    spread = left_sq + right_sq - 2.0 * inner
    return jnp.exp(-sharpness * spread / (left_sq + right_sq + radius_eps)).astype(jnp.bfloat16)


def block_forces(block_rows, ghost_rows):
    rows_f = block_rows.astype(jnp.float32)
    ghosts_f = ghost_rows.astype(jnp.float32)
    own_sq = jnp.sum(rows_f * rows_f, axis=-1)
    ghost_sq = jnp.sum(ghosts_f * ghosts_f, axis=-1)
    own_inner = jnp.einsum("sbw,scw->sbc", rows_f, rows_f, precision=lax.Precision.HIGHEST)
    ghost_inner = jnp.einsum("sbw,smw->sbm", rows_f, ghosts_f, precision=lax.Precision.HIGHEST)
    own_kernel = kernel_weights(own_sq[:, :, None], own_sq[:, None, :], own_inner)
    ghost_kernel = kernel_weights(own_sq[:, :, None], ghost_sq[:, None, :], ghost_inner)
    own_kf = own_kernel.astype(jnp.float32)
    ghost_kf = ghost_kernel.astype(jnp.float32)
    weight_sum = jnp.sum(own_kf, axis=-1) + jnp.sum(ghost_kf, axis=-1)
    pulled = jnp.einsum("sbc,scw->sbw", own_kf, rows_f, precision=lax.Precision.HIGHEST)
    pulled = pulled + jnp.einsum("sbm,smw->sbw", ghost_kf, ghosts_f, precision=lax.Precision.HIGHEST)
    return (force_gain * (pulled - weight_sum[..., None] * rows_f)).astype(jnp.bfloat16)


def flat_index(coord_x, coord_y, coord_z):
    return ((coord_x % N_GX) * N_GY + coord_y % N_GY) * N_GZ + coord_z % N_GZ


def reference(seg_rows, owner_map, ghost_pick, slab_cost):
    hist_x = jnp.sum(slab_cost[:, :, :, 0, :], axis=(0, 1, 2), dtype=jnp.int32)[None]
    hist_y = jnp.sum(slab_cost[:, :, :, 1, :].reshape(2, N_GX // 2, N_GY, N_GZ, NSLAB), axis=(1, 2, 3), dtype=jnp.int32)
    hist_z = jnp.sum(slab_cost[:, :, :, 2, :].reshape(2, N_GX // 2, 2, N_GY // 2, N_GZ, NSLAB), axis=(1, 3, 4), dtype=jnp.int32).reshape(4, NSLAB)
    histogram = jnp.concatenate([hist_x, hist_y, hist_z], axis=0)
    extent = jnp.array([N_GX, N_GY, N_GY, N_GZ, N_GZ, N_GZ, N_GZ], jnp.float32)
    cut_points = bisect_cuts(histogram) * extent

    owners = owner_map[:, 0].reshape(DEVICES, BLK_DEV)
    block_order = jnp.arange(BLK_DEV, dtype=jnp.int32)
    earlier = block_order[:, None] < block_order[None, :]
    same_owner = owners[:, :, None] == owners[:, None, :]
    slot_rank = jnp.sum((same_owner & earlier[None]).astype(jnp.int32), axis=1, dtype=jnp.int32)

    grouped_rows = seg_rows.reshape(DEVICES, BLK_DEV, BLK, W)
    exported = jnp.take_along_axis(grouped_rows, ghost_pick[:, :, None, None], axis=1)
    device = jnp.arange(DEVICES, dtype=jnp.int32)
    along_x = device // (N_GY * N_GZ)
    along_y = (device // N_GZ) % N_GY
    along_z = device % N_GZ
    neighbour = jnp.stack([
        flat_index(along_x - 1, along_y, along_z), flat_index(along_x + 1, along_y, along_z),
        flat_index(along_x, along_y - 1, along_z), flat_index(along_x, along_y + 1, along_z),
        flat_index(along_x, along_y, along_z - 1), flat_index(along_x, along_y, along_z + 1)], axis=1)
    ghost_all = exported[neighbour].reshape(DEVICES, 6 * GH * BLK, W)

    owner_flat = owner_map[:, 0]
    group_size = math.gcd(BLOCKS, 16)

    def per_group(operands):
        rows_group, dest_group = operands
        return block_forces(rows_group, ghost_all[dest_group])

    forces_blocks = lax.map(per_group, (seg_rows.reshape(BLOCKS // group_size, group_size, BLK, W), owner_flat.reshape(BLOCKS // group_size, group_size)))
    forces_blocks = forces_blocks.reshape(BLOCKS, BLK, W)
    source = jnp.arange(BLOCKS, dtype=jnp.int32) // BLK_DEV
    forces = jnp.zeros((DEVICES, DEVICES, CAP, BLK, W), jnp.bfloat16)
    forces = forces.at[owner_flat, source, slot_rank.reshape(-1)].set(forces_blocks)
    return forces, cut_points
```

```python
import functools
import math

import jax
import jax.numpy as jnp
from jax import lax
from jax.experimental import pallas as pl
from jax.experimental.pallas import tpu as pltpu
from jax.sharding import PartitionSpec as P

AXES = ("gx", "gy", "gz")

sharpness = 8.0
force_gain = 2.0
radius_eps = 0.001
LOG2E = 1.0 / math.log(2.0)
LN2 = math.log(2.0)
EXTRA = 8
DIGIT = 64
GROUP = 8


def bisect_cuts(histogram):
    running = jnp.cumsum(histogram, axis=1, dtype=jnp.int32)
    total_cost = running[:, -1]
    below = (2 * running < total_cost[:, None]).astype(jnp.int32)
    position = jnp.sum(below, axis=1, dtype=jnp.int32)
    before = jnp.sum(histogram * below, axis=1, dtype=jnp.int32)
    bins_index = lax.broadcasted_iota(jnp.int32, histogram.shape, 1)
    at_cut = jnp.sum(
        jnp.where(bins_index == position[:, None], histogram, 0), axis=1, dtype=jnp.int32
    )
    remain = (total_cost - 2 * before).astype(jnp.float32)
    return (
        position.astype(jnp.float32) + remain / (2 * at_cut).astype(jnp.float32)
    ) / histogram.shape[1]


def pack_body(owners, seg, tails, first, second, seen, sem, tail_sem):
    blocks, rows, _ = seg.shape
    devices = first.shape[0]
    tail_copy = pltpu.make_async_copy(tails, first.at[:, pl.ds(rows, EXTRA), :], tail_sem)
    tail_copy.start()

    def clear(i, carry):
        seen[i] = 0
        return carry

    lax.fori_loop(0, devices, clear, 0, unroll=8)

    def place(j, carry):
        owner = owners[j]
        rank = seen[owner]
        seen[owner] = rank + 1

        @pl.when(rank == 0)
        def _():
            pltpu.make_async_copy(seg.at[j], first.at[owner, pl.ds(0, rows), :], sem).start()

        @pl.when(rank == 1)
        def _():
            pltpu.make_async_copy(seg.at[j], second.at[owner, pl.ds(0, rows), :], sem).start()

        return carry

    lax.fori_loop(0, blocks, place, 0, unroll=4)
    pltpu.make_async_copy(seg, first.at[:, pl.ds(0, rows), :], sem).wait()
    tail_copy.wait()


def pack(own_owners, seg_rows, tails, devices):
    blocks, rows, width = seg_rows.shape
    out = jax.ShapeDtypeStruct((devices, rows + EXTRA, width), seg_rows.dtype)
    return pl.pallas_call(
        pack_body,
        grid_spec=pltpu.PrefetchScalarGridSpec(
            num_scalar_prefetch=1,
            grid=(1,),
            in_specs=[
                pl.BlockSpec(memory_space=pl.ANY),
                pl.BlockSpec(memory_space=pl.ANY),
            ],
            out_specs=[pl.BlockSpec(out.shape, lambda i, o: (0, 0, 0))] * 2,
            scratch_shapes=[
                pltpu.SMEM((devices,), jnp.int32),
                pltpu.SemaphoreType.DMA,
                pltpu.SemaphoreType.DMA,
            ],
        ),
        out_shape=[out, out],
        compiler_params=pltpu.CompilerParams(vmem_limit_bytes=40 << 20),
        name="pack",
    )(own_owners, seg_rows, tails)


def fill_body(tails, send, out, sem):
    rows = out.shape[1] - EXTRA
    copy = pltpu.make_async_copy(tails, out.at[:, pl.ds(rows, EXTRA), :], sem)
    copy.start()
    copy.wait()


def fill_tails(tails, send):
    return pl.pallas_call(
        fill_body,
        in_specs=[pl.BlockSpec(memory_space=pltpu.VMEM), pl.BlockSpec(memory_space=pl.ANY)],
        out_specs=pl.BlockSpec(memory_space=pl.ANY),
        out_shape=jax.ShapeDtypeStruct(send.shape, send.dtype),
        scratch_shapes=[pltpu.SemaphoreType.DMA],
        input_output_aliases={1: 0},
        name="fill",
    )(tails, send)


def slot_forces(x, ghost_t, ghost_aug, ghost_sq, eye):
    rows = x.shape[0]
    x16 = x * jnp.asarray(2.0 * sharpness, x.dtype)
    own = lax.dot_general(x, x16, (((1,), (1,)), ((), ())), preferred_element_type=jnp.float32)
    diag = jnp.where(eye, own, 0.0)
    scale = LN2 / (2.0 * sharpness)
    sq_row = jnp.sum(diag, axis=0, keepdims=True) * scale
    sq_col = jnp.sum(diag, axis=1, keepdims=True) * scale + LN2 * radius_eps
    shift = sharpness * radius_eps
    top = sharpness * LOG2E

    def weights(inner, right_sq):
        return jnp.exp2((inner + shift) / (sq_col + right_sq) - top).astype(jnp.bfloat16)

    inner = jnp.dot(x, ghost_t, preferred_element_type=jnp.float32)
    own_w = weights(own, sq_row)
    ghost_w = weights(inner, ghost_sq)
    x_aug = jnp.concatenate([x, jnp.ones_like(x)], axis=1)
    total = jnp.dot(ghost_w, ghost_aug, preferred_element_type=jnp.float32)
    total = total + jnp.dot(own_w, x_aug, preferred_element_type=jnp.float32)
    width = x.shape[1]
    pulled, weight_sum = total[:, :width], total[:, width:]
    return force_gain * (pulled - weight_sum * x.astype(jnp.float32))


def force_body(rank, arrivals, recv, ghost_t, ghost_aug, ghost_sq, *rest):
    out = rest[-1]
    rows = out.shape[2]
    step = pl.program_id(0)
    eye = lax.broadcasted_iota(jnp.int32, (rows, rows), 0) == lax.broadcasted_iota(
        jnp.int32, (rows, rows), 1
    )

    def pair(k, carry):
        for m in range(2):
            s = 2 * k + m
            x = recv[s, pl.ds(0, rows), :]
            force = slot_forces(x, ghost_t[...], ghost_aug[...], ghost_sq[...], eye)
            filled = arrivals[step * GROUP + s] > rank
            out[s, 0] = jnp.where(filled, force, 0.0).astype(out.dtype)
        return carry

    lax.fori_loop(0, GROUP // 2, pair, 0)


def pair_forces(rank, arrivals, recv, ghost_t, ghost_aug, ghost_sq, capacity, earlier=None):
    devices, full, width = recv.shape
    rows = full - EXTRA
    pairs = devices * rows * (ghost_t.shape[1] + rows)
    in_specs = [
        pl.BlockSpec((GROUP, full, width), lambda i, a: (i, 0, 0)),
        pl.BlockSpec(ghost_t.shape, lambda i, a: (0, 0)),
        pl.BlockSpec(ghost_aug.shape, lambda i, a: (0, 0)),
        pl.BlockSpec(ghost_sq.shape, lambda i, a: (0, 0)),
    ]
    operands = [arrivals, recv, ghost_t, ghost_aug, ghost_sq]
    aliases = {}
    if earlier is not None:
        in_specs.append(pl.BlockSpec(memory_space=pl.ANY))
        operands.append(earlier)
        aliases = {5: 0}
    return pl.pallas_call(
        functools.partial(force_body, rank),
        grid_spec=pltpu.PrefetchScalarGridSpec(
            num_scalar_prefetch=1,
            grid=(devices // GROUP,),
            in_specs=in_specs,
            out_specs=pl.BlockSpec((GROUP, 1, rows, width), lambda i, a: (i, rank, 0, 0)),
        ),
        out_shape=jax.ShapeDtypeStruct((devices, capacity, rows, width), recv.dtype),
        input_output_aliases=aliases,
        cost_estimate=pl.CostEstimate(
            flops=pairs * width * 6, bytes_accessed=4 * devices * rows * width, transcendentals=2 * pairs
        ),
        compiler_params=pltpu.CompilerParams(vmem_limit_bytes=24 << 20),
        name="forces",
    )(*operands)


def ring(size, step):
    return [(i, (i + step) % size) for i in range(size)]


def per_device(seg_rows, owner_map, ghost_pick, slab_cost):
    count_x = lax.axis_size("gx")
    count_y = lax.axis_size("gy")
    count_z = lax.axis_size("gz")
    devices = count_x * count_y * count_z
    blocks_here, block_rows, width = seg_rows.shape
    capacity = 2
    own_index = lax.axis_index(AXES)
    all_owners = owner_map[:, 0].reshape(devices, blocks_here)
    own_owners = lax.dynamic_index_in_dim(all_owners, own_index, 0, keepdims=False)

    exported = lax.dynamic_index_in_dim(seg_rows, ghost_pick[0, 0], 0, keepdims=False)
    ghosts = []
    for axis, size in (("gx", count_x), ("gy", count_y), ("gz", count_z)):
        ghosts.append(lax.ppermute(exported, axis, ring(size, 1)))
        ghosts.append(lax.ppermute(exported, axis, ring(size, -1)))

    local_cost = slab_cost[0, 0, 0]
    kinds, bins = local_cost.shape
    share = bins // devices
    costs = local_cost.astype(jnp.float32).reshape(kinds * share, devices).T
    tails = jnp.pad(costs[:, None, :], ((0, 0), (0, EXTRA - 1), (0, width - kinds * share)))
    first, second = pack(own_owners, seg_rows, tails.astype(jnp.bfloat16), devices)

    exchange = functools.partial(
        lax.all_to_all, axis_name=AXES, split_axis=0, concat_axis=0, tiled=True
    )
    first = exchange(first)

    costs = first[:, block_rows, : kinds * share].astype(jnp.float32)
    source = lax.broadcasted_iota(jnp.int32, (7, devices), 1)
    row = lax.broadcasted_iota(jnp.int32, (7, devices), 0)
    half = source // (devices // 2)
    quarter = half * 2 + source // (count_z * count_y // 2) % 2
    member = (row == 0) | (row == 1 + half) | (row == 3 + quarter)
    sums = jnp.dot(
        member.astype(jnp.float32), costs, precision=lax.Precision.HIGHEST
    ).reshape(7, kinds, share)
    mine = jnp.concatenate([sums[:1, 0], sums[1:3, 1], sums[3:, 2]], axis=0)
    high = jnp.floor(mine * (1.0 / DIGIT))
    low = mine - DIGIT * high
    tile = jnp.pad(
        jnp.concatenate([high, low], axis=1), ((0, EXTRA - 7), (0, width - 2 * share))
    ).astype(jnp.bfloat16)
    tails = jnp.broadcast_to(tile[None], (devices, EXTRA, width))
    second = exchange(fill_tails(tails, second))

    ghost_set = jnp.concatenate(ghosts, axis=0)
    ghost_float = ghost_set.astype(jnp.float32)
    ghost_sq = jnp.sum(ghost_float * ghost_float, axis=-1)[None] * LN2
    ghost_t = (ghost_set * jnp.asarray(2.0 * sharpness, jnp.bfloat16)).T
    ghost_aug = jnp.concatenate([ghost_set, jnp.ones_like(ghost_set)], axis=1)
    arrivals = jnp.sum((all_owners == own_index).astype(jnp.int32), axis=1, dtype=jnp.int32)

    forces = pair_forces(0, arrivals, first, ghost_t, ghost_aug, ghost_sq, capacity)
    forces = pair_forces(1, arrivals, second, ghost_t, ghost_aug, ghost_sq, capacity, forces)

    digits = second[:, block_rows : block_rows + 7, : 2 * share].astype(jnp.float32)
    whole = DIGIT * digits[:, :, :share] + digits[:, :, share:]
    histogram = whole.transpose(1, 2, 0).reshape(7, bins).astype(jnp.int32)
    extent = jnp.array([count_x, count_y, count_y, count_z, count_z, count_z, count_z], jnp.float32)
    cut_points = bisect_cuts(histogram) * extent
    return (forces[None], cut_points)


def solution(mesh):
    in_specs = (P(AXES, None, None), P(), P(AXES, None), P("gx", "gy", "gz", None, None))
    out_specs = (P(AXES, None, None, None, None), P())
    return jax.shard_map(
        per_device, mesh=mesh, in_specs=in_specs, out_specs=out_specs, check_vma=False
    )
```

```python
import functools
import math

import jax
import jax.numpy as jnp
import ml_dtypes
import numpy as np
from jax import lax
from jax.experimental import pallas as pl
from jax.experimental.pallas import tpu as pltpu
from jax.sharding import PartitionSpec as P

AXES = ("gx", "gy", "gz")

sharpness = 8.0
force_gain = 2.0
radius_eps = 0.001
LN2 = math.log(2.0)
EXTRA = 8
DIGIT = 64
LOW_AT = 64
LOADS = 8
GROUP = 64
ROWS_OF_CUTS = 7


def bf16_terms(value):
    terms = []
    for _ in range(3):
        terms.append(float(np.float32(value).astype(ml_dtypes.bfloat16)))
        value = value - terms[-1]
    return terms


SHIFT = bf16_terms(sharpness * radius_eps)


def pack_body(owners, seg, tails, first, second, held, seen, load_sem, sem, tail_sem):
    blocks, rows, _ = seg.shape
    devices = first.shape[0]
    part = blocks // LOADS
    loads = [
        pltpu.make_async_copy(
            seg.at[pl.ds(k * part, part)], held.at[pl.ds(k * part, part)], load_sem.at[k]
        )
        for k in range(LOADS)
    ]
    for load in loads:
        load.start()
    tail_copy = pltpu.make_async_copy(tails, first.at[:, pl.ds(rows, EXTRA), :], tail_sem)
    tail_copy.start()

    def clear(i, carry):
        seen[i] = 0
        return carry

    lax.fori_loop(0, devices, clear, 0, unroll=8)

    def place(j, carry):
        owner = owners[j]
        rank = seen[owner]
        seen[owner] = rank + 1

        @pl.when(rank == 0)
        def _():
            pltpu.make_async_copy(held.at[j], first.at[owner, pl.ds(0, rows), :], sem).start()

        @pl.when(rank == 1)
        def _():
            pltpu.make_async_copy(held.at[j], second.at[owner, pl.ds(0, rows), :], sem).start()

        return carry

    for k in range(LOADS):
        loads[k].wait()
        lax.fori_loop(k * part, (k + 1) * part, place, 0, unroll=4)
    pltpu.make_async_copy(held, first.at[:, pl.ds(0, rows), :], sem).wait()
    tail_copy.wait()


def pack(own_owners, seg_rows, tails, devices):
    blocks, rows, width = seg_rows.shape
    out = jax.ShapeDtypeStruct((devices, rows + EXTRA, width), seg_rows.dtype)
    return pl.pallas_call(
        pack_body,
        grid_spec=pltpu.PrefetchScalarGridSpec(
            num_scalar_prefetch=1,
            grid=(1,),
            in_specs=[
                pl.BlockSpec(memory_space=pltpu.HBM),
                pl.BlockSpec(tails.shape, lambda i, o: (0, 0, 0)),
            ],
            out_specs=[pl.BlockSpec(memory_space=pltpu.HBM)] * 2,
            scratch_shapes=[
                pltpu.VMEM((blocks, rows, width), seg_rows.dtype),
                pltpu.SMEM((devices,), jnp.int32),
                pltpu.SemaphoreType.DMA((LOADS,)),
                pltpu.SemaphoreType.DMA,
                pltpu.SemaphoreType.DMA,
            ],
        ),
        out_shape=[out, out],
        cost_estimate=pl.CostEstimate(
            flops=1 << 27, bytes_accessed=4 * blocks * rows * width, transcendentals=0
        ),
        name="pack",
    )(own_owners, seg_rows, tails)


def fold_body(layout, recv, send, out, tails, tile, sem):
    devices, group = layout
    rows = out.shape[1] - EXTRA
    width = out.shape[2]
    load = pltpu.make_async_copy(recv.at[:, pl.ds(rows, EXTRA), :], tails, sem.at[0])
    load.start()
    row = lax.broadcasted_iota(jnp.int32, (EXTRA, devices * EXTRA), 0)
    line = lax.broadcasted_iota(jnp.int32, (EXTRA, devices * EXTRA), 1)
    source = line // EXTRA
    half = source // (devices // 2)
    quarter = half * 2 + source // (group // 2) % 2
    member = ((row == 0) | (row == 1 + half) | (row == 3 + quarter)) & (line % EXTRA == 0)
    member = member.astype(jnp.float32).astype(jnp.bfloat16)
    load.wait()
    costs = tails[...].reshape(devices * EXTRA, width)
    sums = jnp.dot(member, costs, preferred_element_type=jnp.float32)
    high = jnp.floor(sums * (1.0 / DIGIT))
    low = sums - DIGIT * high
    lane = lax.broadcasted_iota(jnp.int32, (EXTRA, width), 1)
    digits = jnp.where(lane < LOW_AT, high, pltpu.roll(low, LOW_AT, 1)).astype(jnp.bfloat16)
    tile[...] = jnp.broadcast_to(digits[None], tile.shape)
    store = pltpu.make_async_copy(tile, out.at[:, pl.ds(rows, EXTRA), :], sem.at[1])
    store.start()
    store.wait()


def fold_tails(recv, send, devices, group):
    width = recv.shape[2]
    return pl.pallas_call(
        functools.partial(fold_body, (devices, group)),
        in_specs=[pl.BlockSpec(memory_space=pltpu.HBM)] * 2,
        out_specs=pl.BlockSpec(memory_space=pltpu.HBM),
        out_shape=jax.ShapeDtypeStruct(send.shape, send.dtype),
        scratch_shapes=[
            pltpu.VMEM((devices, EXTRA, width), send.dtype),
            pltpu.VMEM((devices, EXTRA, width), send.dtype),
            pltpu.SemaphoreType.DMA((2,)),
        ],
        input_output_aliases={1: 0},
        name="fold",
    )(recv, send)


def cuts_body(share, extents, recv, out, tails, sem):
    rows = recv.shape[1] - EXTRA
    devices, _, width = tails.shape
    load = pltpu.make_async_copy(recv.at[:, pl.ds(rows, EXTRA), :], tails, sem)
    load.start()
    load.wait()
    digits = tails[...].astype(jnp.float32)
    digits = digits.reshape(devices * EXTRA, width)
    cost = (DIGIT * digits + pltpu.roll(digits, width - LOW_AT, 1)).reshape(devices, EXTRA, width)
    line = lax.broadcasted_iota(jnp.int32, (EXTRA, width), 0)
    lane = lax.broadcasted_iota(jnp.int32, (EXTRA, width), 1)
    kind = jnp.where(line == 0, 0, jnp.where(line < 3, 1, 2))
    valid = (lane // share == kind) & (line < ROWS_OF_CUTS)
    cost = jnp.where(valid[None], cost, 0.0)
    inside = cost
    step = 1
    while step < devices:
        inside = inside + jnp.concatenate(
            [jnp.zeros((step, EXTRA, width), jnp.float32), inside[:-step]], axis=0
        )
        step *= 2
    whole = inside[devices - 1]
    upto = whole
    step = 1
    while step < share:
        upto = upto + jnp.where(lane % share >= step, pltpu.roll(upto, step, 1), 0.0)
        step *= 2
    total = jnp.sum(whole, axis=1, keepdims=True)
    running = inside + (upto - whole)[None]
    below = (2.0 * running < total[None]) & valid[None]
    below = below.astype(jnp.float32)
    position = jnp.sum(jnp.sum(below, axis=0), axis=1, keepdims=True)
    before = jnp.sum(jnp.sum(below * cost, axis=0), axis=1, keepdims=True)
    place = lax.broadcasted_iota(jnp.int32, (devices, EXTRA, width), 0) + (
        lane % share * devices
    )[None]
    hit = place.astype(jnp.float32) == position[None]
    at_cut = jnp.sum(jnp.sum(jnp.where(hit, cost, 0.0), axis=0), axis=1, keepdims=True)
    cut = (position + (total - 2.0 * before) / (2.0 * at_cut)) * (1.0 / (devices * share))
    extent = jnp.where(line == 0, extents[0], jnp.where(line < 3, extents[1], extents[2]))
    out[...] = cut * extent.astype(jnp.float32)


def cuts(recv, share, extents):
    devices, _, width = recv.shape
    return pl.pallas_call(
        functools.partial(cuts_body, share, extents),
        in_specs=[pl.BlockSpec(memory_space=pltpu.HBM)],
        out_specs=pl.BlockSpec(memory_space=pltpu.VMEM),
        out_shape=jax.ShapeDtypeStruct((EXTRA, width), jnp.float32),
        scratch_shapes=[
            pltpu.VMEM((devices, EXTRA, width), recv.dtype),
            pltpu.SemaphoreType.DMA,
        ],
        name="cuts",
    )(recv)[:ROWS_OF_CUTS, 0]


def force_body(rank, group, arrivals, recv, ghost_t, ghost_aug, ghost_sq, *rest):
    out = rest[-7]
    inners, weight_s, columns = rest[-6:-4], rest[-4:-2], rest[-2:]
    rows = out.shape[2]
    width = out.shape[3]
    ghosts = ghost_t.shape[1]
    batches = group // 2
    step = pl.program_id(0)
    scale = LN2 / (2.0 * sharpness)
    eye = lax.broadcasted_iota(jnp.int32, (rows, rows), 0) == lax.broadcasted_iota(
        jnp.int32, (rows, rows), 1
    )
    lane = lax.broadcasted_iota(jnp.int32, (rows, width), 1)
    ones = (lane < 3).astype(jnp.float32).astype(jnp.bfloat16)

    def batch_of(b):
        return 2 * jnp.clip(b, 0, batches - 1)

    def products(b, inner, column):
        s = batch_of(b)
        x = recv[pl.ds(s, 2), pl.ds(0, rows), :].reshape(2 * rows, width)
        x_aug = jnp.concatenate([x, jnp.concatenate([ones, ones], axis=0)], axis=1)
        inner[:, :ghosts] = jnp.dot(x_aug, ghost_t[...], preferred_element_type=jnp.float32)
        for m in range(2):
            mine = x[m * rows : (m + 1) * rows]
            x16 = mine * jnp.asarray(2.0 * sharpness, mine.dtype)
            inner[m * rows : (m + 1) * rows, ghosts:] = lax.dot_general(
                x_aug[m * rows : (m + 1) * rows],
                jnp.concatenate([x16, shift_lanes()], axis=1),
                (((1,), (1,)), ((), ())),
                preferred_element_type=jnp.float32,
            )
            wide = mine.astype(jnp.float32)
            sq = jnp.sum(wide * wide, axis=1, keepdims=True) * LN2 + 0.5 * LN2 * radius_eps
            column[m * rows : (m + 1) * rows] = jnp.broadcast_to(sq, (rows, width))

    def shift_lanes():
        lanes = jnp.zeros((rows, width), jnp.float32)
        for k, term in enumerate(SHIFT):
            lanes = jnp.where(lane == k, term, lanes)
        return lanes.astype(jnp.bfloat16)

    def two(na, da, nb, db):
        r = 1.0 / (da * db)
        return jnp.exp2(na * (r * db)).astype(jnp.bfloat16), jnp.exp2(nb * (r * da)).astype(jnp.bfloat16)

    def weights(inner, column, weight):
        a, b = slice(0, rows), slice(rows, 2 * rows)
        own = [inner[h, ghosts:] for h in (a, b)]
        den = [
            column[h] + jnp.sum(jnp.where(eye, o, 0.0), axis=0, keepdims=True) * scale
            for h, o in zip((a, b), own)
        ]
        weight[a, ghosts:], weight[b, ghosts:] = two(own[0], den[0], own[1], den[1])
        for t in range(0, ghosts, 2 * width):
            p, q = slice(t, t + width), slice(t + width, t + 2 * width)
            weight[:, p], weight[:, q] = two(
                inner[:, p], column[...] + ghost_sq[:, p], inner[:, q], column[...] + ghost_sq[:, q]
            )

    def settle(b, weight):
        s = batch_of(b)
        total = jnp.dot(weight[:, :ghosts], ghost_aug[...], preferred_element_type=jnp.float32)
        for m in range(2):
            here = slice(m * rows, (m + 1) * rows)
            x = recv[s + m, pl.ds(0, rows), :]
            both = total[here] + jnp.dot(
                weight[here, ghosts:],
                jnp.concatenate([x, jnp.ones_like(x)], axis=1),
                preferred_element_type=jnp.float32,
            )
            force = both[:, :width] - both[:, width:] * x.astype(jnp.float32)
            gain = force_gain * math.exp(-sharpness)
            filled = arrivals[step * group + s + m] > rank
            out[s + m, 0] = jnp.where(filled, gain * force, 0.0).astype(out.dtype)

    def body(m, carry):
        b = 2 * m
        for k in range(2):
            e, o = k % 2, (k + 1) % 2
            products(b + k, inners[e], columns[e])
            weights(inners[o], columns[o], weight_s[o])
            settle(b + k - 2, weight_s[e])
        return carry

    lax.fori_loop(0, (batches + 2 + 2 - 1) // 2, body, 0)


def pair_forces(rank, arrivals, recv, ghost_t, ghost_aug, ghost_sq, capacity, earlier=None):
    devices, full, width = recv.shape
    rows = full - EXTRA
    ghosts = ghost_t.shape[1]
    pairs = devices * rows * (ghosts + rows)
    in_specs = [
        pl.BlockSpec((GROUP, full, width), lambda i, a: (i, 0, 0)),
        pl.BlockSpec(ghost_t.shape, lambda i, a: (0, 0)),
        pl.BlockSpec(ghost_aug.shape, lambda i, a: (0, 0)),
        pl.BlockSpec(ghost_sq.shape, lambda i, a: (0, 0)),
    ]
    operands = [arrivals, recv, ghost_t, ghost_aug, ghost_sq]
    aliases = {}
    if earlier is not None:
        in_specs.append(pl.BlockSpec(memory_space=pl.ANY))
        operands.append(earlier)
        aliases = {5: 0}
    return pl.pallas_call(
        functools.partial(force_body, rank, GROUP),
        grid_spec=pltpu.PrefetchScalarGridSpec(
            num_scalar_prefetch=1,
            grid=(devices // GROUP,),
            in_specs=in_specs,
            out_specs=pl.BlockSpec((GROUP, 1, rows, width), lambda i, a: (i, rank, 0, 0)),
            scratch_shapes=[pltpu.VMEM((2 * rows, ghosts + rows), jnp.float32)] * 2
            + [pltpu.VMEM((2 * rows, ghosts + rows), jnp.bfloat16)] * 2
            + [pltpu.VMEM((2 * rows, width), jnp.float32)] * 2,
        ),
        out_shape=jax.ShapeDtypeStruct((devices, capacity, rows, width), recv.dtype),
        input_output_aliases=aliases,
        cost_estimate=pl.CostEstimate(
            flops=pairs * width * 6, bytes_accessed=4 * devices * rows * width, transcendentals=2 * pairs
        ),
        compiler_params=pltpu.CompilerParams(vmem_limit_bytes=32 << 20),
        name="forces",
    )(*operands)


def ring(size, step):
    return [(i, (i + step) % size) for i in range(size)]


def per_device(seg_rows, owner_map, ghost_pick, slab_cost):
    count_x = lax.axis_size("gx")
    count_y = lax.axis_size("gy")
    count_z = lax.axis_size("gz")
    devices = count_x * count_y * count_z
    blocks_here, block_rows, width = seg_rows.shape
    capacity = 2
    own_index = lax.axis_index(AXES)
    all_owners = owner_map[:, 0].reshape(devices, blocks_here)
    own_owners = lax.dynamic_index_in_dim(all_owners, own_index, 0, keepdims=False)

    exported = lax.dynamic_index_in_dim(seg_rows, ghost_pick[0, 0], 0, keepdims=False)
    ghosts = []
    for axis, size in (("gx", count_x), ("gy", count_y), ("gz", count_z)):
        ghosts.append(lax.ppermute(exported, axis, ring(size, 1)))
        ghosts.append(lax.ppermute(exported, axis, ring(size, -1)))

    local_cost = slab_cost[0, 0, 0]
    kinds, bins = local_cost.shape
    share = bins // devices
    costs = local_cost.astype(jnp.float32).reshape(kinds * share, devices).T
    tails = jnp.pad(costs[:, None, :], ((0, 0), (0, EXTRA - 1), (0, width - kinds * share)))
    first, second = pack(own_owners, seg_rows, tails.astype(jnp.bfloat16), devices)
    first, *ghosts = lax.optimization_barrier((first, *ghosts))

    exchange = functools.partial(
        lax.all_to_all, axis_name=AXES, split_axis=0, concat_axis=0, tiled=True
    )
    first = exchange(first)
    second = exchange(fold_tails(first, second, devices, count_y * count_z))

    ghost_set = jnp.concatenate(ghosts, axis=0)
    ghost_float = ghost_set.astype(jnp.float32)
    ghost_sq = jnp.sum(ghost_float * ghost_float, axis=-1)[None] * LN2 + 0.5 * LN2 * radius_eps
    ghost_t = (ghost_set * jnp.asarray(2.0 * sharpness, jnp.bfloat16)).T
    term = jnp.array(SHIFT + [0.0] * (width - len(SHIFT)), jnp.bfloat16)
    ghost_t = jnp.concatenate(
        [ghost_t, jnp.broadcast_to(term[:, None], (width, ghost_t.shape[1]))], axis=0
    )
    ghost_aug = jnp.concatenate([ghost_set, jnp.ones_like(ghost_set)], axis=1)
    arrivals = jnp.sum((all_owners == own_index).astype(jnp.int32), axis=1, dtype=jnp.int32)

    forces = pair_forces(0, arrivals, first, ghost_t, ghost_aug, ghost_sq, capacity)
    forces = pair_forces(1, arrivals, second, ghost_t, ghost_aug, ghost_sq, capacity, forces)
    cut_points = cuts(second, share, (count_x, count_y, count_z))
    return (forces[None], cut_points)


def solution(mesh):
    in_specs = (P(AXES, None, None), P(), P(AXES, None), P("gx", "gy", "gz", None, None))
    out_specs = (P(AXES, None, None, None, None), P())
    return jax.shard_map(
        per_device, mesh=mesh, in_specs=in_specs, out_specs=out_specs, check_vma=False
    )
```

```python
import functools
import math

import jax
import jax.numpy as jnp
import ml_dtypes
import numpy as np
from jax import lax
from jax.experimental import pallas as pl
from jax.experimental.pallas import tpu as pltpu
from jax.sharding import PartitionSpec as P

AXES = ("gx", "gy", "gz")

sharpness = 8.0
force_gain = 2.0
radius_eps = 0.001
LN2 = math.log(2.0)
EXTRA = 8
DIGIT = 64
LOW_AT = 64
LOADS = 8
GROUP = 64
ROWS_OF_CUTS = 7
PHASES = 4


def bf16_terms(value):
    terms = []
    for _ in range(3):
        terms.append(float(np.float32(value).astype(ml_dtypes.bfloat16)))
        value = value - terms[-1]
    return terms


SHIFT = bf16_terms(sharpness * radius_eps)


def pack_body(own, owner_rows, seg, costs, first, second, *scratch):
    held, owners, seen, rolled, tile, load_sem, sem, tail_sem = scratch
    blocks, rows, width = seg.shape
    devices = first.shape[0]
    kinds, bins = costs.shape
    share = bins // devices
    part = blocks // LOADS
    fetch = pltpu.make_async_copy(owner_rows.at[own[0]], owners, tail_sem.at[0])
    fetch.start()
    loads = [
        pltpu.make_async_copy(
            seg.at[pl.ds(k * part, part)], held.at[pl.ds(k * part, part)], load_sem.at[k]
        )
        for k in range(LOADS)
    ]
    for load in loads:
        load.start()

    def clear(i, carry):
        seen[i] = 0
        return carry

    lax.fori_loop(0, devices, clear, 0, unroll=8)
    rolled[...] = jnp.zeros(rolled.shape, jnp.float32)
    for kind in range(kinds):
        for k in range(share):
            line = costs[pl.ds(kind, 1), pl.ds(k * devices, devices)]
            rolled[pl.ds(kind * share + k, 1), :] = line.astype(jnp.float32)
    per_owner = rolled[...].T
    tile[...] = jnp.broadcast_to(per_owner[:, None, :], tile.shape).astype(tile.dtype)
    tail_copy = pltpu.make_async_copy(tile, first.at[:, pl.ds(rows, EXTRA), :], tail_sem.at[1])
    tail_copy.start()

    def place(j, carry):
        owner = owners[j]
        rank = seen[owner]
        seen[owner] = rank + 1

        @pl.when(rank == 0)
        def _():
            pltpu.make_async_copy(held.at[j], first.at[owner, pl.ds(0, rows), :], sem).start()

        @pl.when(rank == 1)
        def _():
            pltpu.make_async_copy(held.at[j], second.at[owner, pl.ds(0, rows), :], sem).start()

        return carry

    fetch.wait()
    for k in range(LOADS):
        loads[k].wait()
        lax.fori_loop(k * part, (k + 1) * part, place, 0, unroll=4)
    pltpu.make_async_copy(held, first.at[:, pl.ds(0, rows), :], sem).wait()
    tail_copy.wait()


def pack(own_index, owner_rows, seg_rows, costs):
    blocks, rows, width = seg_rows.shape
    devices = owner_rows.shape[0]
    out = jax.ShapeDtypeStruct((devices, rows + EXTRA, width), seg_rows.dtype)
    return pl.pallas_call(
        pack_body,
        grid_spec=pltpu.PrefetchScalarGridSpec(
            num_scalar_prefetch=1,
            grid=(1,),
            in_specs=[
                pl.BlockSpec(memory_space=pltpu.HBM),
                pl.BlockSpec(memory_space=pltpu.HBM),
                pl.BlockSpec(costs.shape, lambda i, o: (0, 0)),
            ],
            out_specs=[pl.BlockSpec(memory_space=pltpu.HBM)] * 2,
            scratch_shapes=[
                pltpu.VMEM((blocks, rows, width), seg_rows.dtype),
                pltpu.SMEM((blocks,), jnp.int32),
                pltpu.SMEM((devices,), jnp.int32),
                pltpu.VMEM((width, devices), jnp.float32),
                pltpu.VMEM((devices, EXTRA, width), seg_rows.dtype),
                pltpu.SemaphoreType.DMA((LOADS,)),
                pltpu.SemaphoreType.DMA,
                pltpu.SemaphoreType.DMA((2,)),
            ],
        ),
        out_shape=[out, out],
        cost_estimate=pl.CostEstimate(
            flops=1 << 24, bytes_accessed=4 * blocks * rows * width, transcendentals=0
        ),
        name="pack",
    )(own_index, owner_rows, seg_rows, costs)


def fold_body(layout, recv, send, out, tails, tile, sem):
    devices, group = layout
    rows = out.shape[1] - EXTRA
    width = out.shape[2]
    load = pltpu.make_async_copy(recv.at[:, pl.ds(rows, EXTRA), :], tails, sem.at[0])
    load.start()
    row = lax.broadcasted_iota(jnp.int32, (EXTRA, devices * EXTRA), 0)
    line = lax.broadcasted_iota(jnp.int32, (EXTRA, devices * EXTRA), 1)
    source = line // EXTRA
    half = source // (devices // 2)
    quarter = half * 2 + source // (group // 2) % 2
    member = ((row == 0) | (row == 1 + half) | (row == 3 + quarter)) & (line % EXTRA == 0)
    member = member.astype(jnp.float32).astype(jnp.bfloat16)
    load.wait()
    costs = tails[...].reshape(devices * EXTRA, width)
    sums = jnp.dot(member, costs, preferred_element_type=jnp.float32)
    high = jnp.floor(sums * (1.0 / DIGIT))
    low = sums - DIGIT * high
    lane = lax.broadcasted_iota(jnp.int32, (EXTRA, width), 1)
    digits = jnp.where(lane < LOW_AT, high, pltpu.roll(low, LOW_AT, 1)).astype(jnp.bfloat16)
    tile[...] = jnp.broadcast_to(digits[None], tile.shape)
    store = pltpu.make_async_copy(tile, out.at[:, pl.ds(rows, EXTRA), :], sem.at[1])
    store.start()
    store.wait()


def fold_tails(recv, send, devices, group):
    width = recv.shape[2]
    return pl.pallas_call(
        functools.partial(fold_body, (devices, group)),
        in_specs=[pl.BlockSpec(memory_space=pltpu.HBM)] * 2,
        out_specs=pl.BlockSpec(memory_space=pltpu.HBM),
        out_shape=jax.ShapeDtypeStruct(send.shape, send.dtype),
        scratch_shapes=[
            pltpu.VMEM((devices, EXTRA, width), send.dtype),
            pltpu.VMEM((devices, EXTRA, width), send.dtype),
            pltpu.SemaphoreType.DMA((2,)),
        ],
        input_output_aliases={1: 0},
        name="fold",
    )(recv, send)


def cuts_body(share, extents, recv, out, tails, sem):
    rows = recv.shape[1] - EXTRA
    devices, _, width = tails.shape
    load = pltpu.make_async_copy(recv.at[:, pl.ds(rows, EXTRA), :], tails, sem)
    load.start()
    load.wait()
    digits = tails[...].astype(jnp.float32)
    digits = digits.reshape(devices * EXTRA, width)
    cost = (DIGIT * digits + pltpu.roll(digits, width - LOW_AT, 1)).reshape(devices, EXTRA, width)
    line = lax.broadcasted_iota(jnp.int32, (EXTRA, width), 0)
    lane = lax.broadcasted_iota(jnp.int32, (EXTRA, width), 1)
    kind = jnp.where(line == 0, 0, jnp.where(line < 3, 1, 2))
    valid = (lane // share == kind) & (line < ROWS_OF_CUTS)
    cost = jnp.where(valid[None], cost, 0.0)
    inside = cost
    step = 1
    while step < devices:
        inside = inside + jnp.concatenate(
            [jnp.zeros((step, EXTRA, width), jnp.float32), inside[:-step]], axis=0
        )
        step *= 2
    whole = inside[devices - 1]
    upto = whole
    step = 1
    while step < share:
        upto = upto + jnp.where(lane % share >= step, pltpu.roll(upto, step, 1), 0.0)
        step *= 2
    total = jnp.sum(whole, axis=1, keepdims=True)
    running = inside + (upto - whole)[None]
    below = (2.0 * running < total[None]) & valid[None]
    below = below.astype(jnp.float32)
    position = jnp.sum(jnp.sum(below, axis=0), axis=1, keepdims=True)
    before = jnp.sum(jnp.sum(below * cost, axis=0), axis=1, keepdims=True)
    place = lax.broadcasted_iota(jnp.int32, (devices, EXTRA, width), 0) + (
        lane % share * devices
    )[None]
    hit = place.astype(jnp.float32) == position[None]
    at_cut = jnp.sum(jnp.sum(jnp.where(hit, cost, 0.0), axis=0), axis=1, keepdims=True)
    cut = (position + (total - 2.0 * before) / (2.0 * at_cut)) * (1.0 / (devices * share))
    extent = jnp.where(line == 0, extents[0], jnp.where(line < 3, extents[1], extents[2]))
    cut = cut * extent.astype(jnp.float32)
    for r in range(ROWS_OF_CUTS):
        out[r] = cut[r, 0]


def cuts(recv, share, extents):
    devices, _, width = recv.shape
    return pl.pallas_call(
        functools.partial(cuts_body, share, extents),
        in_specs=[pl.BlockSpec(memory_space=pltpu.HBM)],
        out_specs=pl.BlockSpec(memory_space=pltpu.SMEM),
        out_shape=jax.ShapeDtypeStruct((ROWS_OF_CUTS,), jnp.float32),
        scratch_shapes=[
            pltpu.VMEM((devices, EXTRA, width), recv.dtype),
            pltpu.SemaphoreType.DMA,
        ],
        name="cuts",
    )(recv)


def force_body(rank, group, arrivals, recv, ghost_t, ghost_aug, ghost_sq, *rest):
    out = rest[-7]
    inners, weight_s, columns = rest[-6:-4], rest[-4:-2], rest[-2:]
    rows = out.shape[2]
    width = out.shape[3]
    ghosts = ghost_t.shape[1]
    batches = group // 2
    step = pl.program_id(0)
    scale = LN2 / (2.0 * sharpness)
    eye = lax.broadcasted_iota(jnp.int32, (rows, rows), 0) == lax.broadcasted_iota(
        jnp.int32, (rows, rows), 1
    )
    lane = lax.broadcasted_iota(jnp.int32, (rows, width), 1)
    ones = (lane < 3).astype(jnp.float32).astype(jnp.bfloat16)

    def batch_of(b):
        return 2 * jnp.clip(b, 0, batches - 1)

    def products(b, inner, column):
        s = batch_of(b)
        x = recv[pl.ds(s, 2), pl.ds(0, rows), :].reshape(2 * rows, width)
        x_aug = jnp.concatenate([x, jnp.concatenate([ones, ones], axis=0)], axis=1)
        inner[:, :ghosts] = jnp.dot(x_aug, ghost_t[...], preferred_element_type=jnp.float32)
        for m in range(2):
            mine = x[m * rows : (m + 1) * rows]
            x16 = mine * jnp.asarray(2.0 * sharpness, mine.dtype)
            inner[m * rows : (m + 1) * rows, ghosts:] = lax.dot_general(
                x_aug[m * rows : (m + 1) * rows],
                jnp.concatenate([x16, shift_lanes()], axis=1),
                (((1,), (1,)), ((), ())),
                preferred_element_type=jnp.float32,
            )
            wide = mine.astype(jnp.float32)
            sq = jnp.sum(wide * wide, axis=1, keepdims=True) * LN2 + 0.5 * LN2 * radius_eps
            column[m * rows : (m + 1) * rows] = jnp.broadcast_to(sq, (rows, width))

    def shift_lanes():
        lanes = jnp.zeros((rows, width), jnp.float32)
        for k, term in enumerate(SHIFT):
            lanes = jnp.where(lane == k, term, lanes)
        return lanes.astype(jnp.bfloat16)

    def two(na, da, nb, db):
        r = 1.0 / (da * db)
        return jnp.exp2(na * (r * db)).astype(jnp.bfloat16), jnp.exp2(nb * (r * da)).astype(jnp.bfloat16)

    def weights(inner, column, weight):
        a, b = slice(0, rows), slice(rows, 2 * rows)
        own = [inner[h, ghosts:] for h in (a, b)]
        den = [
            column[h] + jnp.sum(jnp.where(eye, o, 0.0), axis=0, keepdims=True) * scale
            for h, o in zip((a, b), own)
        ]
        weight[a, ghosts:], weight[b, ghosts:] = two(own[0], den[0], own[1], den[1])
        for t in range(0, ghosts, 2 * width):
            p, q = slice(t, t + width), slice(t + width, t + 2 * width)
            weight[:, p], weight[:, q] = two(
                inner[:, p], column[...] + ghost_sq[:, p], inner[:, q], column[...] + ghost_sq[:, q]
            )

    def settle(b, weight):
        s = batch_of(b)
        total = jnp.dot(weight[:, :ghosts], ghost_aug[...], preferred_element_type=jnp.float32)
        for m in range(2):
            here = slice(m * rows, (m + 1) * rows)
            x = recv[s + m, pl.ds(0, rows), :]
            both = total[here] + jnp.dot(
                weight[here, ghosts:],
                jnp.concatenate([x, jnp.ones_like(x)], axis=1),
                preferred_element_type=jnp.float32,
            )
            force = both[:, :width] - both[:, width:] * x.astype(jnp.float32)
            gain = force_gain * math.exp(-sharpness)
            filled = arrivals[step * group + s + m] > rank
            out[s + m, 0] = jnp.where(filled, gain * force, 0.0).astype(out.dtype)

    def body(m, carry):
        for k in range(PHASES):
            e, o = k % 2, (k + 1) % 2
            b = PHASES * m + k
            products(b, inners[e], columns[e])
            weights(inners[o], columns[o], weight_s[o])
            settle(b - 2, weight_s[e])
        return carry

    lax.fori_loop(0, (batches + 2 + PHASES - 1) // PHASES, body, 0)


def pair_forces(rank, arrivals, recv, ghost_t, ghost_aug, ghost_sq, capacity, earlier=None):
    devices, full, width = recv.shape
    rows = full - EXTRA
    ghosts = ghost_t.shape[1]
    pairs = devices * rows * (ghosts + rows)
    in_specs = [
        pl.BlockSpec((GROUP, full, width), lambda i, a: (i, 0, 0)),
        pl.BlockSpec(ghost_t.shape, lambda i, a: (0, 0)),
        pl.BlockSpec(ghost_aug.shape, lambda i, a: (0, 0)),
        pl.BlockSpec(ghost_sq.shape, lambda i, a: (0, 0)),
    ]
    operands = [arrivals, recv, ghost_t, ghost_aug, ghost_sq]
    aliases = {}
    if earlier is not None:
        in_specs.append(pl.BlockSpec(memory_space=pl.ANY))
        operands.append(earlier)
        aliases = {5: 0}
    return pl.pallas_call(
        functools.partial(force_body, rank, GROUP),
        grid_spec=pltpu.PrefetchScalarGridSpec(
            num_scalar_prefetch=1,
            grid=(devices // GROUP,),
            in_specs=in_specs,
            out_specs=pl.BlockSpec((GROUP, 1, rows, width), lambda i, a: (i, rank, 0, 0)),
            scratch_shapes=[pltpu.VMEM((2 * rows, ghosts + rows), jnp.float32)] * 2
            + [pltpu.VMEM((2 * rows, ghosts + rows), jnp.bfloat16)] * 2
            + [pltpu.VMEM((2 * rows, width), jnp.float32)] * 2,
        ),
        out_shape=jax.ShapeDtypeStruct((devices, capacity, rows, width), recv.dtype),
        input_output_aliases=aliases,
        cost_estimate=pl.CostEstimate(
            flops=pairs * width * 6, bytes_accessed=4 * devices * rows * width, transcendentals=2 * pairs
        ),
        compiler_params=pltpu.CompilerParams(vmem_limit_bytes=32 << 20),
        name="forces",
    )(*operands)


def ring(size, step):
    return [(i, (i + step) % size) for i in range(size)]


def per_device(seg_rows, owner_map, ghost_pick, slab_cost):
    count_x = lax.axis_size("gx")
    count_y = lax.axis_size("gy")
    count_z = lax.axis_size("gz")
    devices = count_x * count_y * count_z
    blocks_here, block_rows, width = seg_rows.shape
    capacity = 2
    own_index = lax.axis_index(AXES)
    all_owners = owner_map[:, 0].reshape(devices, blocks_here)
    local_cost = slab_cost[0, 0, 0]
    share = local_cost.shape[1] // devices
    first, second = pack(own_index.astype(jnp.int32)[None], all_owners, seg_rows, local_cost)

    exported = lax.dynamic_index_in_dim(seg_rows, ghost_pick[0, 0], 0, keepdims=False)
    first, exported = lax.optimization_barrier((first, exported))
    ghosts = []
    for axis, size in (("gx", count_x), ("gy", count_y), ("gz", count_z)):
        ghosts.append(lax.ppermute(exported, axis, ring(size, 1)))
        ghosts.append(lax.ppermute(exported, axis, ring(size, -1)))

    exchange = functools.partial(
        lax.all_to_all, axis_name=AXES, split_axis=0, concat_axis=0, tiled=True
    )
    first = exchange(first)
    second = fold_tails(first, second, devices, count_y * count_z)
    second, *ghosts = lax.optimization_barrier((second, *ghosts))
    second = exchange(second)

    ghost_set = jnp.concatenate(ghosts, axis=0)
    ghost_float = ghost_set.astype(jnp.float32)
    ghost_sq = jnp.sum(ghost_float * ghost_float, axis=-1)[None] * LN2 + 0.5 * LN2 * radius_eps
    ghost_t = (ghost_set * jnp.asarray(2.0 * sharpness, jnp.bfloat16)).T
    term = jnp.array(SHIFT + [0.0] * (width - len(SHIFT)), jnp.bfloat16)
    ghost_t = jnp.concatenate(
        [ghost_t, jnp.broadcast_to(term[:, None], (width, ghost_t.shape[1]))], axis=0
    )
    ghost_aug = jnp.concatenate([ghost_set, jnp.ones_like(ghost_set)], axis=1)
    arrivals = jnp.sum((all_owners == own_index).astype(jnp.int32), axis=1, dtype=jnp.int32)

    forces = pair_forces(0, arrivals, first, ghost_t, ghost_aug, ghost_sq, capacity)
    forces = pair_forces(1, arrivals, second, ghost_t, ghost_aug, ghost_sq, capacity, forces)
    cut_points = cuts(second, share, (count_x, count_y, count_z))
    return (forces[None], cut_points)


def solution(mesh):
    in_specs = (P(AXES, None, None), P(), P(AXES, None), P("gx", "gy", "gz", None, None))
    out_specs = (P(AXES, None, None, None, None), P())
    return jax.shard_map(
        per_device, mesh=mesh, in_specs=in_specs, out_specs=out_specs, check_vma=False
    )
```

```python
import functools
import math

import jax
import jax.numpy as jnp
import ml_dtypes
import numpy as np
from jax import lax
from jax.experimental import pallas as pl
from jax.experimental.pallas import tpu as pltpu
from jax.sharding import PartitionSpec as P

AXES = ("gx", "gy", "gz")

sharpness = 8.0
force_gain = 2.0
radius_eps = 0.001
LN2 = math.log(2.0)
EXTRA = 8
DIGIT = 64
LOW_AT = 64
LOADS = 8
GROUP = 64
ROWS_OF_CUTS = 7
BATCH = 8


def bf16_terms(value):
    terms = []
    for _ in range(3):
        terms.append(float(np.float32(value).astype(ml_dtypes.bfloat16)))
        value = value - terms[-1]
    return terms


SHIFT = bf16_terms(sharpness * radius_eps)


def pack_body(own, pick, owner_rows, seg, costs, first, second, exported, *scratch):
    held, owners, seen, rolled, tile, load_sem, sem, tail_sem = scratch
    blocks, rows, width = seg.shape
    devices = first.shape[0]
    part = blocks // LOADS
    fetch = pltpu.make_async_copy(owner_rows.at[own[0]], owners, tail_sem.at[0])
    fetch.start()
    loads = [
        pltpu.make_async_copy(
            seg.at[pl.ds(k * part, part)], held.at[pl.ds(k * part, part)], load_sem.at[k]
        )
        for k in range(LOADS)
    ]
    for load in loads:
        load.start()

    def clear(i, carry):
        seen[i] = 0
        return carry

    lax.fori_loop(0, devices, clear, 0, unroll=8)
    rolled[...] = jnp.zeros(rolled.shape, jnp.float32)
    rolled[: costs.shape[0]] = costs[...].astype(jnp.float32)
    per_owner = rolled[...].T
    tile[...] = jnp.broadcast_to(per_owner[:, None, :], tile.shape).astype(tile.dtype)
    tail_copy = pltpu.make_async_copy(tile, first.at[:, pl.ds(rows, EXTRA), :], tail_sem.at[1])
    tail_copy.start()

    def place(j, carry):
        owner = owners[j]
        rank = seen[owner]
        seen[owner] = rank + 1

        @pl.when(rank == 0)
        def _():
            pltpu.make_async_copy(held.at[j], first.at[owner, pl.ds(0, rows), :], sem).start()

        @pl.when(rank == 1)
        def _():
            pltpu.make_async_copy(held.at[j], second.at[owner, pl.ds(0, rows), :], sem).start()

        return carry

    fetch.wait()
    for k in range(LOADS):
        loads[k].wait()
        lax.fori_loop(k * part, (k + 1) * part, place, 0, unroll=4)
    export = pltpu.make_async_copy(held.at[pick[0]], exported, tail_sem.at[0])
    export.start()
    pltpu.make_async_copy(held, first.at[:, pl.ds(0, rows), :], sem).wait()
    tail_copy.wait()
    export.wait()


def pack(own_index, pick, owner_rows, seg_rows, costs):
    blocks, rows, width = seg_rows.shape
    devices = owner_rows.shape[0]
    out = jax.ShapeDtypeStruct((devices, rows + EXTRA, width), seg_rows.dtype)
    return pl.pallas_call(
        pack_body,
        grid_spec=pltpu.PrefetchScalarGridSpec(
            num_scalar_prefetch=2,
            grid=(1,),
            in_specs=[
                pl.BlockSpec(memory_space=pltpu.HBM),
                pl.BlockSpec(memory_space=pltpu.HBM),
                pl.BlockSpec(costs.shape, lambda i, o, p: (0, 0)),
            ],
            out_specs=[pl.BlockSpec(memory_space=pltpu.HBM)] * 3,
            scratch_shapes=[
                pltpu.VMEM((blocks, rows, width), seg_rows.dtype),
                pltpu.SMEM((blocks,), jnp.int32),
                pltpu.SMEM((devices,), jnp.int32),
                pltpu.VMEM((width, devices), jnp.float32),
                pltpu.VMEM((devices, EXTRA, width), seg_rows.dtype),
                pltpu.SemaphoreType.DMA((LOADS,)),
                pltpu.SemaphoreType.DMA,
                pltpu.SemaphoreType.DMA((2,)),
            ],
        ),
        out_shape=[out, out, jax.ShapeDtypeStruct((rows, width), seg_rows.dtype)],
        cost_estimate=pl.CostEstimate(
            flops=1 << 24, bytes_accessed=4 * blocks * rows * width, transcendentals=0
        ),
        name="pack",
    )(own_index, pick, owner_rows, seg_rows, costs)


def fold_body(layout, recv, send, out, tails, tile, sem):
    devices, group = layout
    rows = out.shape[1] - EXTRA
    width = out.shape[2]
    load = pltpu.make_async_copy(recv.at[:, pl.ds(rows, EXTRA), :], tails, sem.at[0])
    load.start()
    row = lax.broadcasted_iota(jnp.int32, (EXTRA, devices * EXTRA), 0)
    line = lax.broadcasted_iota(jnp.int32, (EXTRA, devices * EXTRA), 1)
    source = line // EXTRA
    half = source // (devices // 2)
    quarter = half * 2 + source // (group // 2) % 2
    member = ((row == 0) | (row == 1 + half) | (row == 3 + quarter)) & (line % EXTRA == 0)
    member = member.astype(jnp.float32).astype(jnp.bfloat16)
    load.wait()
    costs = tails[...].reshape(devices * EXTRA, width)
    sums = jnp.dot(member, costs, preferred_element_type=jnp.float32)
    high = jnp.floor(sums * (1.0 / DIGIT))
    low = sums - DIGIT * high
    lane = lax.broadcasted_iota(jnp.int32, (EXTRA, width), 1)
    digits = jnp.where(lane < LOW_AT, high, pltpu.roll(low, LOW_AT, 1)).astype(jnp.bfloat16)
    tile[...] = jnp.broadcast_to(digits[None], tile.shape)
    store = pltpu.make_async_copy(tile, out.at[:, pl.ds(rows, EXTRA), :], sem.at[1])
    store.start()
    store.wait()


def fold_tails(recv, send, devices, group):
    width = recv.shape[2]
    return pl.pallas_call(
        functools.partial(fold_body, (devices, group)),
        in_specs=[pl.BlockSpec(memory_space=pltpu.HBM)] * 2,
        out_specs=pl.BlockSpec(memory_space=pltpu.HBM),
        out_shape=jax.ShapeDtypeStruct(send.shape, send.dtype),
        scratch_shapes=[
            pltpu.VMEM((devices, EXTRA, width), send.dtype),
            pltpu.VMEM((devices, EXTRA, width), send.dtype),
            pltpu.SemaphoreType.DMA((2,)),
        ],
        input_output_aliases={1: 0},
        name="fold",
    )(recv, send)


def cuts(share, extents, tails, out):
    devices, _, width = tails.shape
    digits = tails[...].astype(jnp.float32)
    digits = digits.reshape(devices * EXTRA, width)
    cost = (DIGIT * digits + pltpu.roll(digits, width - LOW_AT, 1)).reshape(devices, EXTRA, width)
    line = lax.broadcasted_iota(jnp.int32, (EXTRA, width), 0)
    lane = lax.broadcasted_iota(jnp.int32, (EXTRA, width), 1)
    kind = jnp.where(line == 0, 0, jnp.where(line < 3, 1, 2))
    valid = (lane // share == kind) & (line < ROWS_OF_CUTS)
    cost = jnp.where(valid[None], cost, 0.0)
    inside = cost
    step = 1
    while step < devices:
        inside = inside + jnp.concatenate(
            [jnp.zeros((step, EXTRA, width), jnp.float32), inside[:-step]], axis=0
        )
        step *= 2
    whole = inside[devices - 1]
    upto = whole
    step = 1
    while step < share:
        upto = upto + jnp.where(lane % share >= step, pltpu.roll(upto, step, 1), 0.0)
        step *= 2
    total = jnp.sum(whole, axis=1, keepdims=True)
    running = inside + (upto - whole)[None]
    below = (2.0 * running < total[None]) & valid[None]
    below = below.astype(jnp.float32)
    position = jnp.sum(jnp.sum(below, axis=0), axis=1, keepdims=True)
    before = jnp.sum(jnp.sum(below * cost, axis=0), axis=1, keepdims=True)
    place = lax.broadcasted_iota(jnp.int32, (devices, EXTRA, width), 0) + (
        lane % share * devices
    )[None]
    hit = place.astype(jnp.float32) == position[None]
    at_cut = jnp.sum(jnp.sum(jnp.where(hit, cost, 0.0), axis=0), axis=1, keepdims=True)
    cut = (position + (total - 2.0 * before) / (2.0 * at_cut)) * (1.0 / (devices * share))
    extent = jnp.where(line == 0, extents[0], jnp.where(line < 3, extents[1], extents[2]))
    cut = cut * extent.astype(jnp.float32)
    for r in range(ROWS_OF_CUTS):
        out[r] = cut[r, 0]


def force_body(rank, cut_terms, arrivals, recv, ghost_t, ghost_aug, ghost_sq, *rest):
    if cut_terms is None:
        out, rest = rest[0], rest[1:]
    else:
        out, cut_out, tails = rest[1], rest[2], rest[-1]
        rest = rest[3:-1]
    inners, weight_s, columns = rest[0:2], rest[2:4], rest[4:6]
    rows, width = out.shape[2], out.shape[3]
    ghosts = ghost_t.shape[1]
    batches = GROUP // BATCH
    step = pl.program_id(0)
    scale = LN2 / (2.0 * sharpness)
    gain = force_gain * math.exp(-sharpness)
    eye = lax.broadcasted_iota(jnp.int32, (rows, rows), 0) == lax.broadcasted_iota(
        jnp.int32, (rows, rows), 1
    )
    lane = lax.broadcasted_iota(jnp.int32, (rows, width), 1)
    ones = (lane < len(SHIFT)).astype(jnp.float32).astype(jnp.bfloat16)
    shifts = jnp.zeros((rows, width), jnp.float32)
    for k, term in enumerate(SHIFT):
        shifts = jnp.where(lane == k, term, shifts)
    shifts = shifts.astype(jnp.bfloat16)

    def slot(m):
        return slice(m * rows, (m + 1) * rows)

    def products(b, inner, column):
        x = recv[pl.ds(BATCH * b, BATCH), pl.ds(0, rows), :].reshape(BATCH * rows, width)
        x_aug = jnp.concatenate([x, jnp.concatenate([ones] * BATCH, axis=0)], axis=1)
        inner[:, :ghosts] = jnp.dot(x_aug, ghost_t[...], preferred_element_type=jnp.float32)
        for m in range(BATCH):
            mine = x[slot(m)]
            scaled = mine * jnp.asarray(2.0 * sharpness, mine.dtype)
            inner[slot(m), ghosts:] = lax.dot_general(
                x_aug[slot(m)],
                jnp.concatenate([scaled, shifts], axis=1),
                (((1,), (1,)), ((), ())),
                preferred_element_type=jnp.float32,
            )
            wide = mine.astype(jnp.float32)
            sq = jnp.sum(wide * wide, axis=1, keepdims=True) * LN2 + 0.5 * LN2 * radius_eps
            column[slot(m)] = jnp.broadcast_to(sq, (rows, width))

    def two(top_a, den_a, top_b, den_b):
        r = 1.0 / (den_a * den_b)
        return (
            jnp.exp2(top_a * (r * den_b)).astype(jnp.bfloat16),
            jnp.exp2(top_b * (r * den_a)).astype(jnp.bfloat16),
        )

    def weights(inner, column, weight):
        for m in range(BATCH):
            own = inner[slot(m), ghosts:]
            line = jnp.sum(jnp.where(eye, own, 0.0), axis=0, keepdims=True) * scale
            den = column[slot(m)] + line
            h = rows // 2
            upper, lower = two(own[:h], den[:h], own[h:], den[h:])
            weight[m * rows : m * rows + h, ghosts:] = upper
            weight[m * rows + h : (m + 1) * rows, ghosts:] = lower
        for t in range(0, ghosts, 2 * width):
            p, q = slice(t, t + width), slice(t + width, t + 2 * width)
            weight[:, p], weight[:, q] = two(
                inner[:, p], column[...] + ghost_sq[:, p], inner[:, q], column[...] + ghost_sq[:, q]
            )

    def settle(b, weight):
        total = jnp.dot(weight[:, :ghosts], ghost_aug[...], preferred_element_type=jnp.float32)
        for m in range(BATCH):
            at = BATCH * b + m
            x = recv[at, pl.ds(0, rows), :]
            both = total[slot(m)] + jnp.dot(
                weight[slot(m), ghosts:],
                jnp.concatenate([x, jnp.ones_like(x)], axis=1),
                preferred_element_type=jnp.float32,
            )
            force = both[:, :width] - both[:, width:] * x.astype(jnp.float32)
            filled = arrivals[step * GROUP + at] > rank
            out[at, 0] = jnp.where(filled, gain * force, 0.0).astype(out.dtype)

    def body(m, carry):
        products(2 * m, inners[0], columns[0])
        weights(inners[1], columns[1], weight_s[1])
        settle(2 * m - 2, weight_s[0])
        products(2 * m + 1, inners[1], columns[1])
        weights(inners[0], columns[0], weight_s[0])
        settle(2 * m - 1, weight_s[1])
        return carry

    products(0, inners[0], columns[0])
    products(1, inners[1], columns[1])
    weights(inners[0], columns[0], weight_s[0])
    lax.fori_loop(1, batches // 2, body, 0)
    weights(inners[1], columns[1], weight_s[1])
    settle(batches - 2, weight_s[0])
    settle(batches - 1, weight_s[1])

    if cut_terms is not None:
        tails[pl.ds(step * GROUP, GROUP)] = recv[:, pl.ds(rows, EXTRA), :]

        @pl.when(step == pl.num_programs(0) - 1)
        def _():
            cuts(*cut_terms, tails, cut_out)


def pair_forces(
    rank, arrivals, recv, ghost_t, ghost_aug, ghost_sq, capacity, earlier=None, cut_terms=None
):
    devices, full, width = recv.shape
    rows = full - EXTRA
    ghosts = ghost_t.shape[1]
    pairs = devices * rows * (ghosts + rows)
    in_specs = [
        pl.BlockSpec((GROUP, full, width), lambda i, a: (i, 0, 0)),
        pl.BlockSpec(ghost_t.shape, lambda i, a: (0, 0)),
        pl.BlockSpec(ghost_aug.shape, lambda i, a: (0, 0)),
        pl.BlockSpec(ghost_sq.shape, lambda i, a: (0, 0)),
    ]
    operands = [arrivals, recv, ghost_t, ghost_aug, ghost_sq]
    out_specs = [pl.BlockSpec((GROUP, 1, rows, width), lambda i, a: (i, rank, 0, 0))]
    out_shape = [jax.ShapeDtypeStruct((devices, capacity, rows, width), recv.dtype)]
    scratch = (
        [pltpu.VMEM((BATCH * rows, ghosts + rows), jnp.float32)] * 2
        + [pltpu.VMEM((BATCH * rows, ghosts + rows), jnp.bfloat16)] * 2
        + [pltpu.VMEM((BATCH * rows, width), jnp.float32)] * 2
    )
    aliases = {}
    if earlier is not None:
        in_specs.append(pl.BlockSpec(memory_space=pl.ANY))
        operands.append(earlier)
        aliases = {5: 0}
        out_specs.append(pl.BlockSpec(memory_space=pltpu.SMEM))
        out_shape.append(jax.ShapeDtypeStruct((ROWS_OF_CUTS,), jnp.float32))
        scratch.append(pltpu.VMEM((devices, EXTRA, width), recv.dtype))
    return pl.pallas_call(
        functools.partial(force_body, rank, cut_terms),
        grid_spec=pltpu.PrefetchScalarGridSpec(
            num_scalar_prefetch=1,
            grid=(devices // GROUP,),
            in_specs=in_specs,
            out_specs=out_specs,
            scratch_shapes=scratch,
        ),
        out_shape=out_shape,
        input_output_aliases=aliases,
        cost_estimate=pl.CostEstimate(
            flops=pairs * width * 6, bytes_accessed=4 * devices * rows * width, transcendentals=2 * pairs
        ),
        compiler_params=pltpu.CompilerParams(vmem_limit_bytes=40 << 20),
        name="forces",
    )(*operands)


def ring(size, step):
    return [(i, (i + step) % size) for i in range(size)]


def per_device(seg_rows, owner_map, ghost_pick, slab_cost):
    count_x = lax.axis_size("gx")
    count_y = lax.axis_size("gy")
    count_z = lax.axis_size("gz")
    devices = count_x * count_y * count_z
    blocks_here, block_rows, width = seg_rows.shape
    capacity = 2
    own_index = lax.axis_index(AXES)
    all_owners = owner_map[:, 0].reshape(devices, blocks_here)
    share = slab_cost.shape[-1] // devices
    first, second, exported = pack(
        own_index.astype(jnp.int32)[None],
        ghost_pick[0],
        all_owners,
        seg_rows,
        slab_cost.reshape(slab_cost.shape[-2] * share, devices),
    )
    ghosts = []
    for axis, size in (("gx", count_x), ("gy", count_y), ("gz", count_z)):
        ghosts.append(lax.ppermute(exported, axis, ring(size, 1)))
        ghosts.append(lax.ppermute(exported, axis, ring(size, -1)))

    exchange = functools.partial(
        lax.all_to_all, axis_name=AXES, split_axis=0, concat_axis=0, tiled=True
    )
    first = exchange(first)
    second = fold_tails(first, second, devices, count_y * count_z)
    second, *ghosts = lax.optimization_barrier((second, *ghosts))
    second = exchange(second)

    ghost_set = jnp.concatenate(ghosts, axis=0)
    ghost_float = ghost_set.astype(jnp.float32)
    ghost_sq = jnp.sum(ghost_float * ghost_float, axis=-1)[None] * LN2 + 0.5 * LN2 * radius_eps
    ghost_t = (ghost_set * jnp.asarray(2.0 * sharpness, jnp.bfloat16)).T
    term = jnp.array(SHIFT + [0.0] * (width - len(SHIFT)), jnp.bfloat16)
    ghost_t = jnp.concatenate(
        [ghost_t, jnp.broadcast_to(term[:, None], (width, ghost_t.shape[1]))], axis=0
    )
    ghost_aug = jnp.concatenate([ghost_set, jnp.ones_like(ghost_set)], axis=1)
    arrivals = jnp.sum((all_owners == own_index).astype(jnp.int32), axis=1, dtype=jnp.int32)

    (forces,) = pair_forces(0, arrivals, first, ghost_t, ghost_aug, ghost_sq, capacity)
    forces, cut_points = pair_forces(
        1,
        arrivals,
        second,
        ghost_t,
        ghost_aug,
        ghost_sq,
        capacity,
        forces,
        (share, (count_x, count_y, count_z)),
    )
    return (forces[None], cut_points)


def solution(mesh):
    in_specs = (P(AXES, None, None), P(), P(AXES, None), P("gx", "gy", "gz", None, None))
    out_specs = (P(AXES, None, None, None, None), P())
    return jax.shard_map(
        per_device, mesh=mesh, in_specs=in_specs, out_specs=out_specs, check_vma=False
    )
```

```python
import functools
import math

import jax
import jax.numpy as jnp
import ml_dtypes
import numpy as np
from jax import lax
from jax.experimental import pallas as pl
from jax.experimental.pallas import tpu as pltpu
from jax.sharding import Mesh
from jax.sharding import PartitionSpec as P

CHIPS = ("gx", "gy", "gz_0")
CORE = "gz_1"
GZ = ("gz_0", CORE)
AXES = CHIPS + (CORE,)

sharpness = 8.0
force_gain = 2.0
radius_eps = 0.001
LN2 = math.log(2.0)
EXTRA = 8
DIGIT = 64
LOW_AT = 64
LOADS = 8
GROUP = 32
ROWS_OF_CUTS = 7
BATCH = 8


def bf16_terms(value):
    terms = []
    for _ in range(3):
        terms.append(float(np.float32(value).astype(ml_dtypes.bfloat16)))
        value = value - terms[-1]
    return terms


SHIFT = bf16_terms(sharpness * radius_eps)


def pack_body(own, pick, owner_rows, seg, costs, first, near, far, exported, *scratch):
    held, owners, seen, rolled, tile, load_sem, sem, tail_sem = scratch
    blocks, rows, width = seg.shape
    devices = first.shape[0]
    part = blocks // LOADS
    fetch = pltpu.make_async_copy(owner_rows.at[own[0]], owners, tail_sem.at[0])
    fetch.start()
    loads = [
        pltpu.make_async_copy(
            seg.at[pl.ds(k * part, part)], held.at[pl.ds(k * part, part)], load_sem.at[k]
        )
        for k in range(LOADS)
    ]
    for load in loads:
        load.start()

    def clear(i, carry):
        seen[i] = 0
        return carry

    lax.fori_loop(0, devices, clear, 0, unroll=8)
    rolled[...] = jnp.zeros(rolled.shape, jnp.float32)
    rolled[: costs.shape[0]] = costs[...].astype(jnp.float32)
    per_owner = rolled[...].T
    tile[...] = jnp.broadcast_to(per_owner[:, None, :], tile.shape).astype(tile.dtype)
    tail_copy = pltpu.make_async_copy(tile, first.at[:, pl.ds(rows, EXTRA), :], tail_sem.at[1])
    tail_copy.start()

    def place(j, carry):
        owner = owners[j]
        rank = seen[owner]
        seen[owner] = rank + 1

        @pl.when(rank == 0)
        def _():
            pltpu.make_async_copy(held.at[j], first.at[owner, pl.ds(0, rows), :], sem).start()

        again, chip = rank == 1, owner // 2
        beside = (owner - own[0]) % 2 == 0

        @pl.when(again & beside)
        def _():
            pltpu.make_async_copy(held.at[j], near.at[chip], sem).start()

        @pl.when(again & jnp.logical_not(beside))
        def _():
            pltpu.make_async_copy(held.at[j], far.at[chip, pl.ds(0, rows), :], sem).start()

        return carry

    fetch.wait()
    for k in range(LOADS):
        loads[k].wait()
        lax.fori_loop(k * part, (k + 1) * part, place, 0, unroll=4)
    export = pltpu.make_async_copy(held.at[pick[0]], exported, tail_sem.at[0])
    export.start()
    pltpu.make_async_copy(held, first.at[:, pl.ds(0, rows), :], sem).wait()
    tail_copy.wait()
    export.wait()


def pack(own_index, pick, owner_rows, seg_rows, costs):
    blocks, rows, width = seg_rows.shape
    devices = owner_rows.shape[0]
    outs = [
        jax.ShapeDtypeStruct(shape, seg_rows.dtype)
        for shape in (
            (devices, rows + EXTRA, width),
            (devices // 2, rows, width),
            (devices // 2, rows + EXTRA, width),
            (rows, width),
        )
    ]
    return pl.pallas_call(
        pack_body,
        grid_spec=pltpu.PrefetchScalarGridSpec(
            num_scalar_prefetch=2,
            grid=(1,),
            in_specs=[
                pl.BlockSpec(memory_space=pltpu.HBM),
                pl.BlockSpec(memory_space=pltpu.HBM),
                pl.BlockSpec(costs.shape, lambda i, o, p: (0, 0)),
            ],
            out_specs=[pl.BlockSpec(memory_space=pltpu.HBM)] * len(outs),
            scratch_shapes=[
                pltpu.VMEM((blocks, rows, width), seg_rows.dtype),
                pltpu.SMEM((blocks,), jnp.int32),
                pltpu.SMEM((devices,), jnp.int32),
                pltpu.VMEM((width, devices), jnp.float32),
                pltpu.VMEM((devices, EXTRA, width), seg_rows.dtype),
                pltpu.SemaphoreType.DMA((LOADS,)),
                pltpu.SemaphoreType.DMA,
                pltpu.SemaphoreType.DMA((2,)),
            ],
        ),
        out_shape=outs,
        cost_estimate=pl.CostEstimate(
            flops=1 << 24, bytes_accessed=4 * blocks * rows * width, transcendentals=0
        ),
        name="pack",
    )(own_index, pick, owner_rows, seg_rows, costs)


def fold_body(group, recv, out, tails, sem):
    devices = recv.shape[0]
    rows = recv.shape[1] - EXTRA
    width = recv.shape[2]
    load = pltpu.make_async_copy(recv.at[:, pl.ds(rows, EXTRA), :], tails, sem)
    load.start()
    row = lax.broadcasted_iota(jnp.int32, (EXTRA, devices * EXTRA), 0)
    line = lax.broadcasted_iota(jnp.int32, (EXTRA, devices * EXTRA), 1)
    source = line // EXTRA
    half = source // (devices // 2)
    quarter = half * 2 + source // (group // 2) % 2
    member = ((row == 0) | (row == 1 + half) | (row == 3 + quarter)) & (line % EXTRA == 0)
    member = member.astype(jnp.float32).astype(jnp.bfloat16)
    load.wait()
    costs = tails[...].reshape(devices * EXTRA, width)
    sums = jnp.dot(member, costs, preferred_element_type=jnp.float32)
    high = jnp.floor(sums * (1.0 / DIGIT))
    low = sums - DIGIT * high
    lane = lax.broadcasted_iota(jnp.int32, (EXTRA, width), 1)
    out[...] = jnp.where(lane < LOW_AT, high, pltpu.roll(low, LOW_AT, 1)).astype(out.dtype)


def fold(recv, group):
    devices, _, width = recv.shape
    return pl.pallas_call(
        functools.partial(fold_body, group),
        in_specs=[pl.BlockSpec(memory_space=pltpu.HBM)],
        out_specs=pl.BlockSpec(memory_space=pltpu.VMEM),
        out_shape=jax.ShapeDtypeStruct((EXTRA, width), recv.dtype),
        scratch_shapes=[
            pltpu.VMEM((devices, EXTRA, width), recv.dtype),
            pltpu.SemaphoreType.DMA,
        ],
        name="fold",
    )(recv)


def fill_body(used, mine, partner, send, out, tile, sem):
    rows = out.shape[1] - EXTRA
    width = out.shape[2]
    lane = lax.broadcasted_iota(jnp.int32, (EXTRA, width), 1)
    beside = pltpu.roll(partner[...].astype(jnp.float32), used, 1)
    both = jnp.where(lane % LOW_AT < used, mine[...].astype(jnp.float32), beside)
    tile[...] = jnp.broadcast_to(both[None], tile.shape).astype(tile.dtype)
    store = pltpu.make_async_copy(tile, out.at[:, pl.ds(rows, EXTRA), :], sem)
    store.start()
    store.wait()


def fill_tails(used, mine, partner, send):
    chips, _, width = send.shape
    vmem = pl.BlockSpec(memory_space=pltpu.VMEM)
    return pl.pallas_call(
        functools.partial(fill_body, used),
        in_specs=[vmem, vmem, pl.BlockSpec(memory_space=pltpu.HBM)],
        out_specs=pl.BlockSpec(memory_space=pltpu.HBM),
        out_shape=jax.ShapeDtypeStruct(send.shape, send.dtype),
        scratch_shapes=[
            pltpu.VMEM((chips, EXTRA, width), send.dtype),
            pltpu.SemaphoreType.DMA,
        ],
        input_output_aliases={2: 0},
        name="fill",
    )(mine, partner, send)


def cuts(share, extents, core, tails, out):
    chips, _, width = tails.shape
    devices = 2 * chips
    digits = tails[...].astype(jnp.float32).reshape(chips * EXTRA, width)
    cost = DIGIT * digits + pltpu.roll(digits, width - LOW_AT, 1)
    beside = pltpu.roll(cost, width - 3 * share, 1)
    line = lax.broadcasted_iota(jnp.int32, (EXTRA, width), 0)
    lane = lax.broadcasted_iota(jnp.int32, (EXTRA, width), 1)
    kind = jnp.where(line == 0, 0, jnp.where(line < 3, 1, 2))
    valid = (lane // share == kind) & (line < ROWS_OF_CUTS)

    def of_core(k):
        picked = jnp.where(core == k, cost, beside).reshape(chips, EXTRA, width)
        return jnp.where(valid[None], picked, 0.0)

    even, odd = of_core(0), of_core(1)
    inside = even + odd
    step = 1
    while step < chips:
        inside = inside + jnp.concatenate(
            [jnp.zeros((step, EXTRA, width), jnp.float32), inside[:-step]], axis=0
        )
        step *= 2
    whole = inside[chips - 1]
    upto = whole
    step = 1
    while step < share:
        upto = upto + jnp.where(lane % share >= step, pltpu.roll(upto, step, 1), 0.0)
        step *= 2
    total = jnp.sum(whole, axis=1, keepdims=True)
    upto_odd = inside + (upto - whole)[None]
    first_bin = 2 * lax.broadcasted_iota(jnp.int32, (chips, EXTRA, width), 0) + (
        lane % share * devices
    )[None]

    def added(values):
        return jnp.sum(jnp.sum(values, axis=0), axis=1, keepdims=True)

    position, before = 0.0, 0.0
    sides = ((even, upto_odd - odd, first_bin), (odd, upto_odd, first_bin + 1))
    for side, running, _ in sides:
        below = ((2.0 * running < total[None]) & valid[None]).astype(jnp.float32)
        position = position + added(below)
        before = before + added(below * side)
    at_cut = 0.0
    for side, _, place in sides:
        at_cut = at_cut + added(jnp.where(place.astype(jnp.float32) == position[None], side, 0.0))
    cut = (position + (total - 2.0 * before) / (2.0 * at_cut)) * (1.0 / (devices * share))
    extent = jnp.where(line == 0, extents[0], jnp.where(line < 3, extents[1], extents[2]))
    cut = cut * extent.astype(jnp.float32)
    for r in range(ROWS_OF_CUTS):
        out[r] = cut[r, 0]


def force_body(rank, base, cut_terms, arrivals, side, recv, ghost_t, ghost_aug, ghost_sq, *rest):
    if cut_terms is not None:
        tails, rest = rest[-1], rest[:-1]
    out = rest[0 if rank == 0 and base == 0 else 1]
    inners, weight_s, columns = rest[-6:-4], rest[-4:-2], rest[-2:]
    rows, width = out.shape[3], out.shape[4]
    ghosts = ghost_t.shape[1]
    batches = GROUP // BATCH
    step = pl.program_id(0)
    scale = LN2 / (2.0 * sharpness)
    gain = force_gain * math.exp(-sharpness)
    eye = lax.broadcasted_iota(jnp.int32, (rows, rows), 0) == lax.broadcasted_iota(
        jnp.int32, (rows, rows), 1
    )
    lane = lax.broadcasted_iota(jnp.int32, (rows, width), 1)
    ones = (lane < len(SHIFT)).astype(jnp.float32).astype(jnp.bfloat16)
    shifts = jnp.zeros((rows, width), jnp.float32)
    for k, term in enumerate(SHIFT):
        shifts = jnp.where(lane == k, term, shifts)
    shifts = shifts.astype(jnp.bfloat16)

    def slot(m):
        return slice(m * rows, (m + 1) * rows)

    def products(b, inner, column):
        x = recv[pl.ds(BATCH * b, BATCH), pl.ds(0, rows), :].reshape(BATCH * rows, width)
        x_aug = jnp.concatenate([x, jnp.concatenate([ones] * BATCH, axis=0)], axis=1)
        inner[:, :ghosts] = jnp.dot(x_aug, ghost_t[...], preferred_element_type=jnp.float32)
        for m in range(BATCH):
            mine = x[slot(m)]
            scaled = mine * jnp.asarray(2.0 * sharpness, mine.dtype)
            inner[slot(m), ghosts:] = lax.dot_general(
                x_aug[slot(m)],
                jnp.concatenate([scaled, shifts], axis=1),
                (((1,), (1,)), ((), ())),
                preferred_element_type=jnp.float32,
            )
            wide = mine.astype(jnp.float32)
            sq = jnp.sum(wide * wide, axis=1, keepdims=True) * LN2 + 0.5 * LN2 * radius_eps
            column[slot(m)] = jnp.broadcast_to(sq, (rows, width))

    def two(top_a, den_a, top_b, den_b):
        r = 1.0 / (den_a * den_b)
        return (
            jnp.exp2(top_a * (r * den_b)).astype(jnp.bfloat16),
            jnp.exp2(top_b * (r * den_a)).astype(jnp.bfloat16),
        )

    def weights(inner, column, weight):
        for m in range(BATCH):
            own = inner[slot(m), ghosts:]
            line = jnp.sum(jnp.where(eye, own, 0.0), axis=0, keepdims=True) * scale
            den = column[slot(m)] + line
            h = rows // 2
            upper, lower = two(own[:h], den[:h], own[h:], den[h:])
            weight[m * rows : m * rows + h, ghosts:] = upper
            weight[m * rows + h : (m + 1) * rows, ghosts:] = lower
        for t in range(0, ghosts, 2 * width):
            p, q = slice(t, t + width), slice(t + width, t + 2 * width)
            weight[:, p], weight[:, q] = two(
                inner[:, p], column[...] + ghost_sq[:, p], inner[:, q], column[...] + ghost_sq[:, q]
            )

    def settle(b, weight):
        total = jnp.dot(weight[:, :ghosts], ghost_aug[...], preferred_element_type=jnp.float32)
        for m in range(BATCH):
            at = BATCH * b + m
            x = recv[at, pl.ds(0, rows), :]
            both = total[slot(m)] + jnp.dot(
                weight[slot(m), ghosts:],
                jnp.concatenate([x, jnp.ones_like(x)], axis=1),
                preferred_element_type=jnp.float32,
            )
            force = both[:, :width] - both[:, width:] * x.astype(jnp.float32)
            if rank:
                place, source = (at, 0, 0), 2 * (step * GROUP + at) + side[0]
            else:
                place, source = (at // 2, at % 2, 0), (base + step) * GROUP + at
            filled = arrivals[source] > rank
            out[place] = jnp.where(filled, gain * force, 0.0).astype(out.dtype)

    def body(m, carry):
        products(2 * m, inners[0], columns[0])
        weights(inners[1], columns[1], weight_s[1])
        settle(2 * m - 2, weight_s[0])
        products(2 * m + 1, inners[1], columns[1])
        weights(inners[0], columns[0], weight_s[0])
        settle(2 * m - 1, weight_s[1])
        return carry

    products(0, inners[0], columns[0])
    products(1, inners[1], columns[1])
    weights(inners[0], columns[0], weight_s[0])
    lax.fori_loop(1, batches // 2, body, 0)
    weights(inners[1], columns[1], weight_s[1])
    settle(batches - 2, weight_s[0])
    settle(batches - 1, weight_s[1])

    if cut_terms is not None:
        tails[pl.ds(step * GROUP, GROUP)] = recv[:, pl.ds(rows, EXTRA), :]

        @pl.when(step == pl.num_programs(0) - 1)
        def _():
            cuts(*cut_terms, 1 - side[0], tails, rest[2])


def pair_forces(rank, part, arrivals, side, recv, rows, ghosts, earlier=None, cut_terms=None):
    base, steps = part
    _, full, width = recv.shape
    slots = steps * GROUP
    ghost_t, ghost_aug, ghost_sq = ghosts
    partners = ghost_t.shape[1] + rows
    chips = arrivals.shape[0] // 2
    in_specs = [
        pl.BlockSpec((GROUP, full, width), lambda i, a, c: (base + i, 0, 0)),
        pl.BlockSpec(ghost_t.shape, lambda i, a, c: (0, 0)),
        pl.BlockSpec(ghost_aug.shape, lambda i, a, c: (0, 0)),
        pl.BlockSpec(ghost_sq.shape, lambda i, a, c: (0, 0)),
    ]
    operands = [arrivals, side, recv, ghost_t, ghost_aug, ghost_sq]
    if rank:
        out_spec = pl.BlockSpec((GROUP, 1, 1, rows, width), lambda i, a, c: (i, c[0], rank, 0, 0))
    else:
        out_spec = pl.BlockSpec((GROUP // 2, 2, 1, rows, width), lambda i, a, c: (base + i, 0, 0, 0, 0))
    out_specs = [out_spec]
    out_shape = [jax.ShapeDtypeStruct((chips, 2, 2, rows, width), recv.dtype)]
    aliases, scratch = {}, []
    if earlier is not None:
        in_specs.append(pl.BlockSpec(memory_space=pl.ANY))
        operands.append(earlier)
        aliases = {6: 0}
    if cut_terms is not None:
        out_specs.append(pl.BlockSpec(memory_space=pltpu.SMEM))
        out_shape.append(jax.ShapeDtypeStruct((ROWS_OF_CUTS,), jnp.float32))
        scratch = [pltpu.VMEM((chips, EXTRA, width), recv.dtype)]
    pairs = slots * rows * partners
    return pl.pallas_call(
        functools.partial(force_body, rank, base, cut_terms),
        grid_spec=pltpu.PrefetchScalarGridSpec(
            num_scalar_prefetch=2,
            grid=(steps,),
            in_specs=in_specs,
            out_specs=out_specs,
            scratch_shapes=[pltpu.VMEM((BATCH * rows, partners), jnp.float32)] * 2
            + [pltpu.VMEM((BATCH * rows, partners), jnp.bfloat16)] * 2
            + [pltpu.VMEM((BATCH * rows, width), jnp.float32)] * 2
            + scratch,
        ),
        out_shape=out_shape,
        input_output_aliases=aliases,
        cost_estimate=pl.CostEstimate(
            flops=pairs * width * 6, bytes_accessed=4 * slots * rows * width, transcendentals=2 * pairs
        ),
        compiler_params=pltpu.CompilerParams(vmem_limit_bytes=62 << 20),
        name="forces",
    )(*operands)


def ring(size, step):
    return [(i, (i + step) % size) for i in range(size)]


def per_device(seg_rows, owner_map, ghost_pick, slab_cost):
    count_x = lax.axis_size("gx")
    count_y = lax.axis_size("gy")
    count_z = lax.axis_size(GZ)
    devices = count_x * count_y * count_z
    blocks_here, block_rows, width = seg_rows.shape
    own_index = lax.axis_index(AXES).astype(jnp.int32)
    core = lax.axis_index(CORE).astype(jnp.int32)
    all_owners = owner_map[:, 0].reshape(devices, blocks_here)
    kinds, bins = slab_cost.shape[-2:]
    share = bins // devices
    first, near, far, exported = pack(
        own_index[None],
        ghost_pick[0],
        all_owners,
        seg_rows,
        slab_cost.reshape(kinds * share, devices),
    )
    first, exported, far = lax.optimization_barrier((first, exported, far))
    swap = [(0, 1), (1, 0)]
    far = lax.ppermute(far, CORE, swap)
    ghosts = []
    for axis, size in (("gx", count_x), ("gy", count_y), (GZ, count_z)):
        ghosts.append(lax.ppermute(exported, axis, ring(size, 1)))
        ghosts.append(lax.ppermute(exported, axis, ring(size, -1)))

    exchange = functools.partial(lax.all_to_all, split_axis=0, concat_axis=0, tiled=True)
    first = exchange(first, AXES)
    near, *ghosts = lax.optimization_barrier((near, *ghosts))
    near = exchange(near, CHIPS)

    mine = fold(first, count_y * count_z)
    partner = lax.ppermute(mine, CORE, swap)
    ghost_set = jnp.concatenate(ghosts, axis=0)
    ghost_float = ghost_set.astype(jnp.float32)
    ghost_sq = jnp.sum(ghost_float * ghost_float, axis=-1)[None] * LN2 + 0.5 * LN2 * radius_eps
    ghost_t = (ghost_set * jnp.asarray(2.0 * sharpness, jnp.bfloat16)).T
    term = jnp.array(SHIFT + [0.0] * (width - len(SHIFT)), jnp.bfloat16)
    ghost_t = jnp.concatenate(
        [ghost_t, jnp.broadcast_to(term[:, None], (width, ghost_t.shape[1]))], axis=0
    )
    ghost_aug = jnp.concatenate([ghost_set, jnp.ones_like(ghost_set)], axis=1)
    arrivals = jnp.sum((all_owners == own_index).astype(jnp.int32), axis=1, dtype=jnp.int32)
    ghosts = (ghost_t, ghost_aug, ghost_sq)
    far = fill_tails(kinds * share, mine, partner, far)
    first, far = lax.optimization_barrier((first, far))
    steps = devices // GROUP
    some = (steps + 1) // 2
    (forces,) = pair_forces(0, (0, some), arrivals, core[None], first, block_rows, ghosts)
    far, forces = lax.optimization_barrier((far, forces))
    far = exchange(far, CHIPS)
    (forces,) = pair_forces(
        0, (some, steps - some), arrivals, core[None], first, block_rows, ghosts, forces
    )
    steps = devices // 2 // GROUP
    (forces,) = pair_forces(
        1, (0, steps), arrivals, core[None], near, block_rows, ghosts, forces
    )
    forces, cut_points = pair_forces(
        1,
        (0, steps),
        arrivals,
        1 - core[None],
        far,
        block_rows,
        ghosts,
        forces,
        (share, (count_x, count_y, count_z)),
    )
    return (forces.reshape(1, devices, 2, block_rows, width), cut_points)


def solution(mesh):
    finer = Mesh(
        mesh.devices.reshape(mesh.shape["gx"], mesh.shape["gy"], mesh.shape["gz"] // 2, 2), AXES
    )
    in_specs = (P(AXES, None, None), P(), P(AXES, None), P("gx", "gy", GZ, None, None))
    out_specs = (P(AXES, None, None, None, None), P())
    return jax.shard_map(
        per_device, mesh=finer, in_specs=in_specs, out_specs=out_specs, check_vma=False
    )
```
